32 devices in a mesh: ell: 4 (over y, x), blk: 8 (over z, core).
Axes of the slice: x: 2, y: 2, z: 4, core: 2. Of those that a mesh axis runs over, the one named last changes fastest.
Arguments:
- wigner: bfloat16 [8, 17, 2101248], P(None, None, ('ell', 'blk')), may hold values from -6 to 6
- sky_alm: float32 [2, 2101248], P(None, ('ell', 'blk')), may hold values from -0.03125 to 0.03125
- beam_blm: float32 [2, 17, 2048], replicated, may hold values from -4.25 to 4.25
- slot_col: int32 [2101248], P(('ell', 'blk')), may hold values from -1 to 255, as said below
- slot_ell: int32 [2101248], P(('ell', 'blk')), may hold values from 0 to 2047, as said below
- order_of_column: int32 [2048], replicated, may hold values from 0 to 2047, as said below
Outputs:
- conv_cube: float32 [8, 32, 4096], P('ell', 'blk')
The draws below stay inside these ranges and needn't reach their ends.
Inputs may be any that keep to these rules, and one draw needn't show every extreme that they name: `slot_col`: slot block b (slots b * 65664 to b * 65664 + 65663) belongs to ell index b // 8 and blk index b % 8; at most 65568 slots of a block are live, and some blocks have exactly that many. `slot_ell`: every pair (l, m) with m <= l < 2048 stands in exactly one live slot; within a blk group, higher ell indices hold degrees no lower than those of lower ell indices. `order_of_column`: A permutation of 0 to 2047; every blk group's orders hold the same number of pairs.
All inputs are finite; a program needn't handle non-finite values.
Results may differ from the reference program's by a relative error of at most 0.0029.
Values sent between devices are 32-bit elements; how exact they have to be, the bound alone decides.
A program may use at most 256 MiB of HBM per device.

```python
import math
import jax
import jax.numpy as jnp
from jax import lax

L = 2048
K = 17
NPSI = 32
THETA = 8
NPHI = 4096
M_DEV = 256
LIVE_MOST = 65568
SLOT_DEV = 65664
SLOTS = 2101248
N_ELL = 4
N_BLK = 8


def pair_tables(key):
    half = L // 2
    fold = L // (2 * N_BLK)
    blocks = N_ELL * N_BLK
    cols = L // N_BLK
    order = jax.random.permutation(jax.random.fold_in(key, 101), half)
    lower = order.reshape(N_BLK, fold)
    grouped = jnp.concatenate([lower, L - 1 - lower], axis=1).astype(jnp.int32)
    col_keys = jax.random.split(jax.random.fold_in(key, 102), N_BLK)
    col_perm = jax.vmap(lambda inner_key: jax.random.permutation(inner_key, cols))(col_keys)
    order_table = jnp.take_along_axis(grouped, col_perm.astype(jnp.int32), axis=1)
    degrees = jnp.arange(L, dtype=jnp.int32)
    valid = order_table[:, None, :] <= degrees[None, :, None]
    flat_valid = valid.reshape(N_BLK, L * cols)
    position = jnp.cumsum(flat_valid.astype(jnp.int32), axis=1) - 1
    ell_index = position // LIVE_MOST
    offset = jnp.clip(position % LIVE_MOST, 0, SLOT_DEV - 1)
    group_index = jnp.arange(N_BLK, dtype=jnp.int32)[:, None]
    block = jnp.clip(ell_index * N_BLK + group_index, 0, blocks - 1)
    shuffle_keys = jax.random.split(jax.random.fold_in(key, 103), blocks)
    shuffles = jax.vmap(lambda inner_key: jax.random.permutation(inner_key, SLOT_DEV))(shuffle_keys).astype(jnp.int32)
    slot = block * SLOT_DEV + shuffles[block, offset]
    target = jnp.where(flat_valid, slot, blocks * SLOT_DEV).reshape(-1)
    col_values = jnp.broadcast_to(jnp.arange(cols, dtype=jnp.int32)[None, None, :], (N_BLK, L, cols)).reshape(-1)
    ell_values = jnp.broadcast_to(degrees[None, :, None], (N_BLK, L, cols)).reshape(-1)
    slot_col = jnp.full((blocks * SLOT_DEV,), -1, jnp.int32).at[target].set(col_values, mode='drop')
    slot_ell = jnp.zeros((blocks * SLOT_DEV,), jnp.int32).at[target].set(ell_values, mode='drop')
    return (order_table.reshape(L), slot_col, slot_ell)


def draw_order_of_column(key, part):
    return pair_tables(key)[0]


def draw_slot_col(key, part):
    return pair_tables(key)[1]


def draw_slot_ell(key, part):
    return pair_tables(key)[2]


def draw_beam_blm(key, part):
    degrees = jnp.arange(L, dtype=jnp.float32)
    scale = (2.0 * (degrees + 1.0)) ** (-0.5)
    base = jnp.clip(jax.random.normal(key, (2, K, L), jnp.float32), -6.0, 6.0)
    return (base * scale[None, None, :]).astype(jnp.float32)


def level_of(key, shape, pieces, low, top_value):
    def one(dim, blocks):
        draws = jax.random.uniform(jax.random.fold_in(jax.random.fold_in(key, 6), dim), (blocks,), jnp.float32, low / len(pieces), top_value / len(pieces))
        return jnp.repeat(jnp.exp(draws), shape[dim] // blocks).reshape((-1,) + (1,) * (len(shape) - dim - 1))

    gain = one(*pieces[0])
    for cut in pieces[1:]:
        gain = gain * one(*cut)
    return gain


def scatter_about(rng, shape, deviation, reach, shards=(), held_as=jnp.bfloat16):
    array = jax.random.normal(rng, shape, jnp.float32) * deviation
    if len(shards) > 0:
        array = level_of(rng, shape, shards, -0.22, 0.18) * array
    return jnp.clip(array, min=-reach, max=reach).astype(held_as)


def setup_inputs(seed: int = 0) -> dict:
    key_of = jax.random.split(jax.random.key(seed), 7)
    wigner = scatter_about(key_of[0], (THETA, K, SLOTS), 1.0, 6.0, ((2, 32),))
    sky_alm = scatter_about(key_of[1], (2, SLOTS), (L * K) ** -0.5, 0.03125, ((1, 32),), jnp.float32)
    beam_blm = draw_beam_blm(jax.random.fold_in(key_of[6], 71), 0)
    slot_col = draw_slot_col(jax.random.fold_in(key_of[6], 71), 0)
    slot_ell = draw_slot_ell(jax.random.fold_in(key_of[6], 71), 0)
    order_of_column = draw_order_of_column(jax.random.fold_in(key_of[6], 71), 0)
    return dict(wigner=wigner, sky_alm=sky_alm, beam_blm=beam_blm, slot_col=slot_col, slot_ell=slot_ell, order_of_column=order_of_column)


def phase_table(rows, cols, period):
    product = (jnp.arange(rows, dtype=jnp.int32)[:, None] * jnp.arange(cols, dtype=jnp.int32)[None, :]) % period
    angle = product.astype(jnp.float32) * (2.0 * math.pi / period)
    return jnp.cos(angle), jnp.sin(angle)


def psi_table(order_count, samples):
    cosines, sine_terms = phase_table(order_count, samples, samples)
    real_row = jnp.stack([cosines, sine_terms], axis=1)
    imag_row = jnp.stack([-sine_terms, cosines], axis=1)
    return jnp.stack([real_row, imag_row], axis=0)


def reference(wigner, sky_alm, beam_blm, slot_col, slot_ell, order_of_column):
    block_count = SLOTS // SLOT_DEV

    def accumulate(running, block_index):
        first_slot = block_index * SLOT_DEV
        wig_rows = lax.dynamic_slice_in_dim(wigner, first_slot, SLOT_DEV, 2).astype(jnp.float32)
        alm_part = lax.dynamic_slice_in_dim(sky_alm, first_slot, SLOT_DEV, 1)
        columns = lax.dynamic_slice_in_dim(slot_col, first_slot, SLOT_DEV, 0)
        degrees = lax.dynamic_slice_in_dim(slot_ell, first_slot, SLOT_DEV, 0)
        beam_slots = jnp.take(beam_blm, degrees, axis=2)
        coeffs = jnp.stack([alm_part[0] * beam_slots[0] - alm_part[1] * beam_slots[1],
                            alm_part[0] * beam_slots[1] + alm_part[1] * beam_slots[0]])
        values = (wig_rows[:, None] * coeffs[None]).astype(jnp.bfloat16)
        values = lax.optimization_barrier(values).astype(jnp.float32)
        group = (block_index % N_BLK).astype(jnp.int32)
        global_col = group * M_DEV + jnp.maximum(columns, 0)
        orders = jnp.where(columns >= 0, jnp.take(order_of_column, global_col), L).astype(jnp.int32)
        flat = values.reshape(THETA * 2 * K, SLOT_DEV).T
        return running + jax.ops.segment_sum(flat, orders, num_segments=L + 1)[:L], None

    totals, _ = lax.scan(accumulate, jnp.zeros((L, THETA * 2 * K), jnp.float32),
                         jnp.arange(block_count, dtype=jnp.int32))
    harmonic = totals.T.reshape(THETA, 2, K, L)
    psi_field = jnp.einsum("trkc,rksp->tspc", harmonic, psi_table(K, NPSI), precision=lax.Precision.HIGHEST)
    complex_field = psi_field[:, 0] + 1j * psi_field[:, 1]
    padded = jnp.pad(complex_field, ((0, 0), (0, 0), (0, NPHI - L)))
    return (jnp.real(jnp.fft.ifft(padded, axis=-1)) * NPHI).astype(jnp.float32)
```

```python
import functools
import math

import jax
import jax.numpy as jnp
from jax import lax
from jax.experimental import pallas as pl
from jax.experimental.pallas import tpu as pltpu
from jax.sharding import PartitionSpec as P

NPSI = 32
LANES = 128
SUBLANES = 8
MXU = 256
MXU_ROWS = 1024
TRIP = 16


def phase_table(rows, cols, period):
    product = (
        jnp.arange(rows, dtype=jnp.int32)[:, None]
        * jnp.arange(cols, dtype=jnp.int32)[None, :]
        % period
    )
    angle = product.astype(jnp.float32) * (2.0 * math.pi / period)
    return (jnp.cos(angle), jnp.sin(angle))


def psi_table(order_count, samples):
    cosines, sine_terms = phase_table(order_count, samples, samples)
    real_row = jnp.stack([cosines, sine_terms], axis=1)
    imag_row = jnp.stack([-sine_terms, cosines], axis=1)
    return jnp.stack([real_row, imag_row], axis=0)


def to_phi(fields, order_of_column):
    cycles = fields.shape[0]
    samples = fields.shape[2]
    degrees = fields.shape[3]
    period = 2 * degrees
    inner = 2 ** ((period.bit_length() - 1) // 2)
    outer = period // inner
    highest = lax.Precision.HIGH
    high_part = order_of_column // inner
    low_part = order_of_column % inner
    turns = high_part[:, None] * jnp.arange(outer, dtype=jnp.int32)[None, :] % outer
    angle = turns.astype(jnp.float32) * (2.0 * math.pi / outer)
    cos_first = jnp.cos(angle)
    sin_first = jnp.sin(angle)
    select = (low_part[:, None] == jnp.arange(inner, dtype=jnp.int32)[None, :]).astype(jnp.float32)
    real_in = fields[:, 0]
    imag_in = fields[:, 1]
    weighted_re = real_in[..., None] * cos_first - imag_in[..., None] * sin_first
    weighted_im = real_in[..., None] * sin_first + imag_in[..., None] * cos_first
    first_re = jnp.einsum("tpcj,cv->tpvj", weighted_re, select, precision=highest)
    first_im = jnp.einsum("tpcj,cv->tpvj", weighted_im, select, precision=highest)
    cos_twist, sin_twist = phase_table(inner, outer, period)
    twist_re = first_re * cos_twist - first_im * sin_twist
    twist_im = first_re * sin_twist + first_im * cos_twist
    cos_last, sin_last = phase_table(inner, inner, inner)
    result = jnp.einsum("tpvj,vw->tpwj", twist_re, cos_last, precision=highest) - jnp.einsum(
        "tpvj,vw->tpwj", twist_im, sin_last, precision=highest
    )
    return result.reshape(cycles, samples, period)


def lane_pick(table, index):
    return lax.gather(
        table,
        index[..., None],
        lax.GatherDimensionNumbers(
            offset_dims=(),
            collapsed_slice_dims=(1,),
            start_index_map=(1,),
            operand_batching_dims=(0,),
            start_indices_batching_dims=(0,),
        ),
        slice_sizes=(1, 1),
        mode=lax.GatherScatterMode.PROMISE_IN_BOUNDS,
    )


def pick_span(col_ref, ell_ref, tiles):
    live = col_ref[...] >= 0
    degree = ell_ref[...]
    last = tiles * LANES - 1
    top = jnp.max(jnp.where(live, degree, 0).astype(jnp.float32)).astype(jnp.int32)
    low = jnp.min(jnp.where(live, degree, last).astype(jnp.float32)).astype(jnp.int32)
    return low // LANES, top // LANES


def sums_kernel(
    orders, cols, trips, wig_hbm, sky_ref, col_ref, ell_ref, beam_ref, out_ref, wig_buf, tail_buf, *scratch
):
    coeff_refs, sems, tail_sem = scratch[0:2], scratch[2], scratch[3]
    cycles = wig_hbm.shape[1]
    tiles = beam_ref.shape[2] // LANES
    slot_tiles = col_ref.shape[0]
    rest = slot_tiles - trips * TRIP
    depth = wig_buf.shape[0]
    half = orders * cycles
    by_rows = 2 * half > MXU_ROWS

    def wig_copy(trip, slot):
        lanes = pl.ds(pl.multiple_of(trip * (TRIP * LANES), LANES), TRIP * LANES)
        return pltpu.make_async_copy(wig_hbm.at[:, :, lanes], wig_buf.at[slot], sems.at[slot])

    def tail_copy():
        lanes = pl.ds(trips * TRIP * LANES, rest * LANES)
        return pltpu.make_async_copy(wig_hbm.at[:, :, lanes], tail_buf, tail_sem)

    for trip in range(min(depth - 1, trips)):
        wig_copy(trip, trip).start()
    if rest:
        tail_copy().start()

    low, top = pick_span(col_ref, ell_ref, tiles)
    span = top - low + 1
    row16 = lax.broadcasted_iota(jnp.int32, (16, LANES), 0).astype(jnp.float32).astype(jnp.bfloat16)

    def coeffs(count, first, tile, rows, coeff):
        degree = ell_ref[pl.ds(tile, rows), :]
        sky_re = sky_ref[pl.ds(2 * tile, rows, stride=2), :]
        sky_im = sky_ref[pl.ds(2 * tile + 1, rows, stride=2), :]
        high = (degree >> 7) - first
        index = degree & (LANES - 1)
        here = [high == t for t in range(1, count)]

        def pick(part, order):
            picked = None
            for t in range(count):
                lanes = pl.ds(pl.multiple_of((first + t) * LANES, LANES), LANES)
                entry = jnp.broadcast_to(beam_ref[part, pl.ds(order, 1), lanes], (rows, LANES))
                value = lane_pick(entry, index)
                picked = value if t == 0 else jnp.where(here[t - 1], value, picked)
            return picked

        for order in range(orders):
            real = pick(0, order)
            imag = pick(1, order)
            coeff[order, pl.ds(0, rows), :] = sky_re * real - sky_im * imag
            coeff[orders + order, pl.ds(0, rows), :] = sky_re * imag + sky_im * real

    def values(wig, coeff, part, start, line):
        out = []
        for order in range(orders):
            here = wig[order, :, pl.ds(start, LANES)].astype(jnp.float32)
            row = coeff[part * orders + order, pl.ds(line, 1), :]
            out.append(here * jnp.broadcast_to(row, (cycles, LANES)))
        return jnp.concatenate(out, axis=0)

    def hot(tile):
        line = jnp.broadcast_to(col_ref[pl.ds(tile, 1), :], (16, LANES))
        away = line.astype(jnp.float32).astype(jnp.bfloat16) - row16
        one, zero = jnp.ones_like(away), jnp.zeros_like(away)
        out = [jnp.where(away == jnp.bfloat16(16 * g), one, zero) for g in range(cols // 16)]
        out += [zero] * (MXU // 16 - cols // 16)
        return jnp.concatenate(out, axis=0)

    def body(acc0, acc1):
        accs = (acc0, acc1)
        if by_rows:
            work = lambda i: [(0, i % 2, (0,)), (1, i % 2, (1,))]
        else:
            work = lambda i: [(i % 2, i // 2 % 2, (0, 1))]

        ahead = 1 if by_rows else 2

        def push(i, tile, count=2):
            left = hot(tile)
            right = hot(tile + 1) if count == 2 else jnp.zeros_like(left)
            both = jnp.concatenate([left, right], axis=1)
            for mxu, register, _ in work(i):
                pltpu.matmul_push_rhs(both, register, mxu, transpose=True)

        def multiply(i, wig, coeff, start, line, count=2):
            for mxu, register, parts in work(i):
                blocks = []
                for part in parts:
                    left = values(wig, coeff, part, start, line)
                    if count == 2:
                        right = values(wig, coeff, part, start + LANES, line + 1)
                    else:
                        right = jnp.zeros_like(left)
                    blocks.append(jnp.concatenate([left, right], axis=1))
                block = blocks[0] if len(blocks) == 1 else jnp.concatenate(blocks, axis=0)
                pltpu.matmul_acc_lhs(accs[mxu], block, load_staged_rhs=register)

        pairs = TRIP // 2
        tail_pairs = -(-rest // 2)

        def tail_size(i):
            return min(2, rest - 2 * i)

        def run(count, first):
            coeffs(count, first, 0, SUBLANES, coeff_refs[0])
            for i in range(ahead):
                push(i, 2 * i)

            def trip_body(trip, last):
                slot = lax.rem(trip, depth)
                wig_copy(trip, slot).wait()
                wig = wig_buf.at[slot]
                base = trip * TRIP
                for i in range(pairs):
                    which = 2 * i // SUBLANES
                    if 2 * i % SUBLANES == 0:
                        later = base + (which + 1) * SUBLANES
                        if not last or which + 1 < TRIP // SUBLANES:
                            coeffs(count, first, pl.multiple_of(later, SUBLANES), SUBLANES, coeff_refs[1 - which])
                        else:
                            lines = min(rest, SUBLANES)
                            if lines:
                                coeffs(count, first, trips * TRIP, lines, coeff_refs[0])
                    multiply(i, wig, coeff_refs[which], 2 * i * LANES, 2 * i % SUBLANES)
                    after = i + ahead
                    if not last or after < pairs:
                        push(after, base + 2 * after)
                    elif after - pairs < tail_pairs:
                        push(after, base + 2 * after, tail_size(after - pairs))

            @pl.loop(0, trips - 1)
            def _(trip):
                @pl.when(trip + depth - 1 < trips)
                def _():
                    wig_copy(trip + depth - 1, lax.rem(trip + depth - 1, depth)).start()

                trip_body(trip, False)

            trip_body(trips - 1, True)
            if rest:
                tail_copy().wait()
            for i in range(tail_pairs):
                tile = trips * TRIP + 2 * i
                if 2 * i == SUBLANES:
                    coeffs(count, first, tile, rest - SUBLANES, coeff_refs[1])
                which = 2 * i // SUBLANES
                multiply(pairs + i, tail_buf, coeff_refs[which], 2 * i * LANES, 2 * i % SUBLANES, tail_size(i))
                if ahead + i < tail_pairs:
                    push(pairs + i + ahead, tile + 2 * ahead, tail_size(i + ahead))

        counts = sorted({min(c, tiles) for c in (4, 9)})
        below = 0
        for count in counts:
            first = jnp.minimum(low, tiles - count)

            @pl.when((span > below) & (span <= count) if below else span <= count)
            def _():
                run(count, first)

            below = count
        if below < tiles:

            @pl.when(span > below)
            def _():
                run(tiles, 0)

        if by_rows:
            out_ref[pl.ds(0, half), :] = pltpu.matmul_pop(acc0)[:, :cols]
            out_ref[pl.ds(half, half), :] = pltpu.matmul_pop(acc1)[:, :cols]
        else:
            out_ref[...] = (pltpu.matmul_pop(acc0) + pltpu.matmul_pop(acc1))[:, :cols]

    rows = half if by_rows else 2 * half
    pl.run_scoped(body, pltpu.ACC(0)((rows, MXU), jnp.float32), pltpu.ACC(1)((rows, MXU), jnp.float32))


def order_sums(wigner, sky_alm, beam_blm, slot_col, slot_ell, cols):
    cycles, orders, slots = wigner.shape
    tiles = slots // LANES
    trips = tiles // TRIP
    rest = tiles - trips * TRIP
    depth = 8
    rows = orders * 2 * cycles
    whole = lambda shape: pl.BlockSpec(shape, lambda: (0,) * len(shape))
    sky = sky_alm.reshape(2, tiles, LANES).transpose(1, 0, 2).reshape(2 * tiles, LANES)
    wig = pltpu.with_memory_space_constraint(wigner.transpose(1, 0, 2), pltpu.HBM)
    return pl.pallas_call(
        functools.partial(sums_kernel, orders, cols, trips),
        out_shape=jax.ShapeDtypeStruct((rows, cols), jnp.float32),
        in_specs=[
            pl.BlockSpec(memory_space=pltpu.HBM),
            whole((2 * tiles, LANES)),
            whole((tiles, LANES)),
            whole((tiles, LANES)),
            whole(beam_blm.shape),
        ],
        out_specs=whole((rows, cols)),
        scratch_shapes=[
            pltpu.VMEM((depth, orders, cycles, TRIP * LANES), jnp.bfloat16),
            pltpu.VMEM((orders, cycles, max(rest, 1) * LANES), jnp.bfloat16),
            *[pltpu.VMEM((2 * orders, SUBLANES, LANES), jnp.float32) for _ in range(2)],
            pltpu.SemaphoreType.DMA((depth,)),
            pltpu.SemaphoreType.DMA,
        ],
        compiler_params=pltpu.CompilerParams(vmem_limit_bytes=48 * 1024 * 1024),
        name="order_sums",
    )(wig, sky, slot_col.reshape(tiles, LANES), slot_ell.reshape(tiles, LANES), beam_blm)


def on_device(wigner, sky_alm, beam_blm, slot_col, slot_ell, order_of_column):
    cycle_total = wigner.shape[0]
    order_count = wigner.shape[1]
    blk_count = lax.axis_size("blk")
    col_count = order_of_column.shape[0] // blk_count
    col_sums = order_sums(wigner, sky_alm, beam_blm, slot_col, slot_ell, col_count)
    by_cycle = col_sums.reshape(2, order_count, cycle_total, col_count).transpose(2, 0, 1, 3)
    ell_count = lax.axis_size("ell")
    partials = by_cycle.reshape((ell_count, cycle_total // ell_count) + by_cycle.shape[1:])
    summed = lax.all_to_all(partials, "ell", split_axis=0, concat_axis=0, tiled=True).sum(axis=0)
    owned = jnp.einsum(
        "trkc,rksp->tspc",
        summed,
        psi_table(order_count, NPSI),
        precision=lax.Precision.HIGHEST,
    )
    return to_phi(
        lax.all_to_all(owned, "blk", split_axis=2, concat_axis=3, tiled=True), order_of_column
    )


def solution(mesh):
    return jax.shard_map(
        on_device,
        mesh=mesh,
        in_specs=(
            P(None, None, ("ell", "blk")),
            P(None, ("ell", "blk")),
            P(),
            P(("ell", "blk")),
            P(("ell", "blk")),
            P(),
        ),
        out_specs=P("ell", "blk", None),
        check_vma=False,
    )
```

```python
import functools
import math

import jax
import jax.numpy as jnp
import numpy as np
from jax import lax
from jax.experimental import pallas as pl
from jax.experimental.pallas import tpu as pltpu
from jax.sharding import PartitionSpec as P

NPSI = 32
LANES = 128
SUBLANES = 8
MXU = 256
MXU_ROWS = 1024
TRIP = 16
MESH = pl.DeviceIdType.MESH


def round_up(value, step):
    return -(-value // step) * step


def lane_pick(table, index):
    return lax.gather(
        table,
        index[..., None],
        lax.GatherDimensionNumbers(
            offset_dims=(),
            collapsed_slice_dims=(1,),
            start_index_map=(1,),
            operand_batching_dims=(0,),
            start_indices_batching_dims=(0,),
        ),
        slice_sizes=(1, 1),
        mode=lax.GatherScatterMode.PROMISE_IN_BOUNDS,
    )


REAL_STEP = 1 << 19
IMAG_SHIFT = 13
POWER_BITS = 6
LEAST_POWER = 62
FULL = 4094.0


def largest(blocks):
    most = functools.reduce(jnp.maximum, [jnp.abs(block) for block in blocks])
    return jnp.max(most, axis=(0, 1), keepdims=True)


def pack_beam(real_ref, imag_ref, table_ref):
    orders, degrees = table_ref.shape
    most = jnp.maximum(largest([real_ref[...], imag_ref[...]]), 1e-30)
    unit = jnp.broadcast_to(1.0 / most, (orders, LANES))
    for tile in range(degrees // LANES):
        lanes = pl.ds(tile * LANES, LANES)
        real, imag = real_ref[:, lanes] * unit, imag_ref[:, lanes] * unit
        size = jnp.maximum(jnp.abs(real), jnp.abs(imag))
        power = jnp.floor(jnp.log2(size)) + 1.0
        power = jnp.minimum(jnp.maximum(power, -float(LEAST_POWER)), 1.0)
        grow = jnp.exp2(-power) * FULL
        code = (power + float(LEAST_POWER)).astype(jnp.int32)
        below = code.astype(jnp.float32) * (1.0 / 64.0)
        imag_code = jnp.floor(imag * grow - below + 0.5).astype(jnp.int32)
        low = ((imag_code & 0x1FFF) << POWER_BITS) + code
        below = low.astype(jnp.float32) * (1.0 / REAL_STEP)
        real_code = jnp.floor(real * grow - below + 0.5).astype(jnp.int32)
        table_ref[:, lanes] = (real_code << 19) + low
    return most


def pick_span(col_ref, ell_ref, tiles):
    live = col_ref[...] >= 0
    degree = ell_ref[...]
    last = tiles * LANES - 1
    top = jnp.max(jnp.where(live, degree, 0).astype(jnp.float32)).astype(jnp.int32)
    low = jnp.min(jnp.where(live, degree, last).astype(jnp.float32)).astype(jnp.int32)
    return low // LANES, top // LANES


def sums_kernel(orders, cols, trips, wig_hbm, sky_hbm, col_hbm, ell_hbm, beam_hbm, out_ref, *scratch):
    wig_buf, tail_buf, sky_ref, col_ref, ell_ref, real_ref, imag_ref, table_ref = scratch[0:8]
    coeff_refs, sems, once = scratch[8:10], scratch[10], scratch[11]
    cycles = wig_hbm.shape[1]
    tiles = table_ref.shape[1] // LANES
    slot_tiles = col_ref.shape[0]
    rest = slot_tiles - trips * TRIP
    depth = wig_buf.shape[0]
    half = orders * cycles
    by_rows = 2 * half > MXU_ROWS

    def wig_copy(trip, slot):
        lanes = pl.ds(pl.multiple_of(trip * (TRIP * LANES), LANES), TRIP * LANES)
        return pltpu.make_async_copy(wig_hbm.at[:, :, lanes], wig_buf.at[slot], sems.at[slot])

    rest_lanes = pl.ds(trips * TRIP * LANES, rest * LANES)
    ell_copy = pltpu.make_async_copy(ell_hbm, ell_ref, once.at[0])
    col_copy = pltpu.make_async_copy(col_hbm, col_ref, once.at[1])
    real_copy = pltpu.make_async_copy(beam_hbm.at[:, 0, :], real_ref, once.at[2])
    imag_copy = pltpu.make_async_copy(beam_hbm.at[:, 1, :], imag_ref, once.at[3])
    sky_copy = pltpu.make_async_copy(sky_hbm, sky_ref, once.at[4])
    for copy in (real_copy, imag_copy, col_copy, ell_copy, sky_copy):
        copy.start()
    for trip in range(min(depth - 1, trips)):
        wig_copy(trip, trip).start()
    if rest:
        tail_copy = pltpu.make_async_copy(wig_hbm.at[:, :, rest_lanes], tail_buf, once.at[5])
        tail_copy.start()

    real_copy.wait()
    imag_copy.wait()
    most = pack_beam(real_ref, imag_ref, table_ref)
    unit = jnp.broadcast_to(most * (1.0 / (REAL_STEP * FULL)), (SUBLANES, LANES))
    col_copy.wait()
    ell_copy.wait()
    low, top = pick_span(col_ref, ell_ref, tiles)
    span = top - low + 1
    sky_copy.wait()
    row16 = lax.broadcasted_iota(jnp.int32, (16, LANES), 0).astype(jnp.float32).astype(jnp.bfloat16)

    def coeffs(count, first, tile, rows, coeff):
        degree = ell_ref[pl.ds(tile, rows), :]
        lanes = pl.ds(pl.multiple_of(tile * LANES, LANES), rows * LANES)
        sky_re = sky_ref[pl.ds(0, 1), lanes].reshape(rows, LANES) * unit[:rows]
        sky_im = sky_ref[pl.ds(1, 1), lanes].reshape(rows, LANES) * unit[:rows]
        high = (degree >> 7) - first
        index = degree & (LANES - 1)
        here = [high == t for t in range(1, count)]
        for order in range(orders):
            word = None
            for t in range(count):
                lanes = pl.ds(pl.multiple_of((first + t) * LANES, LANES), LANES)
                entry = jnp.broadcast_to(table_ref[pl.ds(order, 1), lanes], (rows, LANES))
                value = lane_pick(entry, index)
                word = value if t == 0 else jnp.where(here[t - 1], value, word)
            real = word.astype(jnp.float32)
            imag = (word << IMAG_SHIFT).astype(jnp.float32)
            power = jnp.exp2((word & (2**POWER_BITS - 1)).astype(jnp.float32) - float(LEAST_POWER))
            real, imag = real * power, imag * power
            coeff[order, pl.ds(0, rows), :] = sky_re * real - sky_im * imag
            coeff[orders + order, pl.ds(0, rows), :] = sky_re * imag + sky_im * real

    def values(wig, coeff, part, start, line):
        out = []
        for order in range(orders):
            here = wig[order, :, pl.ds(start, LANES)].astype(jnp.float32)
            row = coeff[part * orders + order, pl.ds(line, 1), :]
            out.append(here * jnp.broadcast_to(row, (cycles, LANES)))
        return jnp.concatenate(out, axis=0)

    def hot(tile):
        line = jnp.broadcast_to(col_ref[pl.ds(tile, 1), :], (16, LANES))
        away = line.astype(jnp.float32).astype(jnp.bfloat16) - row16
        one, zero = jnp.ones_like(away), jnp.zeros_like(away)
        out = [jnp.where(away == jnp.bfloat16(16 * g), one, zero) for g in range(cols // 16)]
        out += [zero] * (MXU // 16 - cols // 16)
        return jnp.concatenate(out, axis=0)

    def body(acc0, acc1):
        accs = (acc0, acc1)
        if by_rows:
            work = lambda i: [(0, i % 2, (0,)), (1, i % 2, (1,))]
        else:
            work = lambda i: [(i % 2, i // 2 % 2, (0, 1))]

        ahead = 1 if by_rows else 2

        def push(i, tile, count=2):
            left = hot(tile)
            right = hot(tile + 1) if count == 2 else jnp.zeros_like(left)
            both = jnp.concatenate([left, right], axis=1)
            for mxu, register, _ in work(i):
                pltpu.matmul_push_rhs(both, register, mxu, transpose=True)

        def multiply(i, wig, coeff, start, line, count=2):
            for mxu, register, parts in work(i):
                blocks = []
                for part in parts:
                    left = values(wig, coeff, part, start, line)
                    if count == 2:
                        right = values(wig, coeff, part, start + LANES, line + 1)
                    else:
                        right = jnp.zeros_like(left)
                    blocks.append(jnp.concatenate([left, right], axis=1))
                block = blocks[0] if len(blocks) == 1 else jnp.concatenate(blocks, axis=0)
                pltpu.matmul_acc_lhs(accs[mxu], block, load_staged_rhs=register)

        pairs = TRIP // 2
        tail_pairs = -(-rest // 2)

        def tail_size(i):
            return min(2, rest - 2 * i)

        def run(count, first):
            coeffs(count, first, 0, SUBLANES, coeff_refs[0])
            for i in range(ahead):
                push(i, 2 * i)

            def trip_body(trip, last):
                slot = lax.rem(trip, depth)
                wig_copy(trip, slot).wait()
                wig = wig_buf.at[slot]
                base = trip * TRIP
                for i in range(pairs):
                    which = 2 * i // SUBLANES
                    if 2 * i % SUBLANES == 0:
                        later = base + (which + 1) * SUBLANES
                        if not last or which + 1 < TRIP // SUBLANES:
                            coeffs(count, first, pl.multiple_of(later, SUBLANES), SUBLANES, coeff_refs[1 - which])
                        else:
                            lines = min(rest, SUBLANES)
                            if lines:
                                coeffs(count, first, trips * TRIP, lines, coeff_refs[0])
                    multiply(i, wig, coeff_refs[which], 2 * i * LANES, 2 * i % SUBLANES)
                    after = i + ahead
                    if not last or after < pairs:
                        push(after, base + 2 * after)
                    elif after - pairs < tail_pairs:
                        push(after, base + 2 * after, tail_size(after - pairs))

            @pl.loop(0, trips - 1)
            def _(trip):
                @pl.when(trip + depth - 1 < trips)
                def _():
                    wig_copy(trip + depth - 1, lax.rem(trip + depth - 1, depth)).start()

                trip_body(trip, False)

            trip_body(trips - 1, True)
            if rest:
                tail_copy.wait()
            for i in range(tail_pairs):
                tile = trips * TRIP + 2 * i
                if 2 * i == SUBLANES:
                    coeffs(count, first, tile, rest - SUBLANES, coeff_refs[1])
                which = 2 * i // SUBLANES
                multiply(pairs + i, tail_buf, coeff_refs[which], 2 * i * LANES, 2 * i % SUBLANES, tail_size(i))
                if ahead + i < tail_pairs:
                    push(pairs + i + ahead, tile + 2 * ahead, tail_size(i + ahead))

        counts = sorted({min(c, tiles) for c in (4, 9)})
        below = 0
        for count in counts:
            first = jnp.minimum(low, tiles - count)

            @pl.when((span > below) & (span <= count) if below else span <= count)
            def _():
                run(count, first)

            below = count
        if below < tiles:

            @pl.when(span > below)
            def _():
                run(tiles, 0)

        groups = round_up(2 * orders, SUBLANES)
        width = out_ref.shape[2]
        sums = [pltpu.matmul_pop(acc0), pltpu.matmul_pop(acc1)]
        if not by_rows:
            sums = [sums[0] + sums[1]]
        sums = jnp.concatenate(sums, axis=0)
        for piece in range(cols // width):
            lanes = slice(piece * width, (piece + 1) * width)
            for cycle in range(cycles):
                if groups > 2 * orders:
                    pad = pl.ds(cycle * groups + 2 * orders, groups - 2 * orders)
                    out_ref[piece, pad, :] = jnp.zeros((groups - 2 * orders, width), jnp.float32)
            for row in range(2 * orders):
                for cycle in range(0, cycles, SUBLANES):
                    here = pl.ds(cycle * groups + row, SUBLANES, stride=groups)
                    start = row * cycles + cycle
                    out_ref[piece, here, :] = sums[start : start + SUBLANES, lanes]

    rows = half if by_rows else 2 * half
    pl.run_scoped(body, pltpu.ACC(0)((rows, MXU), jnp.float32), pltpu.ACC(1)((rows, MXU), jnp.float32))


def order_sums(wigner, sky_alm, beam_blm, slot_col, slot_ell, cols):
    cycles, orders, slots = wigner.shape
    degrees = beam_blm.shape[2]
    tiles = slots // LANES
    trips = tiles // TRIP
    rest = tiles - trips * TRIP
    depth = 8
    width = min(cols, LANES)
    shape = (cols // width, cycles * round_up(2 * orders, SUBLANES), width)
    in_hbm = lambda x: pltpu.with_memory_space_constraint(x, pltpu.HBM)
    return pl.pallas_call(
        functools.partial(sums_kernel, orders, cols, trips),
        out_shape=jax.ShapeDtypeStruct(shape, jnp.float32),
        in_specs=[pl.BlockSpec(memory_space=pltpu.HBM)] * 5,
        out_specs=pl.BlockSpec(memory_space=pltpu.VMEM),
        scratch_shapes=[
            pltpu.VMEM((depth, orders, cycles, TRIP * LANES), jnp.bfloat16),
            pltpu.VMEM((orders, cycles, max(rest, 1) * LANES), jnp.bfloat16),
            pltpu.VMEM((2, slots), jnp.float32),
            pltpu.VMEM((tiles, LANES), jnp.int32),
            pltpu.VMEM((tiles, LANES), jnp.int32),
            pltpu.VMEM((orders, degrees), jnp.float32),
            pltpu.VMEM((orders, degrees), jnp.float32),
            pltpu.VMEM((orders, degrees), jnp.int32),
            *[pltpu.VMEM((2 * orders, SUBLANES, LANES), jnp.float32) for _ in range(2)],
            pltpu.SemaphoreType.DMA((depth,)),
            pltpu.SemaphoreType.DMA((6,)),
        ],
        compiler_params=pltpu.CompilerParams(vmem_limit_bytes=32 * 1024 * 1024),
        name="order_sums",
    )(
        in_hbm(wigner.transpose(1, 0, 2)),
        in_hbm(sky_alm),
        in_hbm(slot_col.reshape(tiles, LANES)),
        in_hbm(slot_ell.reshape(tiles, LANES)),
        in_hbm(beam_blm.transpose(1, 0, 2)),
    )


def split(value):
    high = value.astype(jnp.bfloat16)
    return high, (value - high.astype(jnp.float32)).astype(jnp.bfloat16)


def split_table(table):
    high, low = split(jnp.asarray(table, jnp.float32))
    return jnp.stack([high, low])


def product(left, right):
    dot = functools.partial(jnp.dot, preferred_element_type=jnp.float32)
    return dot(left[0], right[0]) + dot(left[0], right[1]) + dot(left[1], right[0])


def psi_rows(orders, blks, turns, samples):
    groups, lines = round_up(2 * orders, SUBLANES), round_up(turns * samples, SUBLANES)
    table = np.zeros((blks, 2, lines, turns, groups))
    sample = np.arange(blks * samples).reshape(blks, samples)
    angle = 2.0 * np.pi * (sample[..., None] * np.arange(orders) % (blks * samples)) / (blks * samples)
    for turn in range(turns):
        rows = slice(turn * samples, (turn + 1) * samples)
        table[:, 0, rows, turn, :orders] = np.cos(angle)
        table[:, 0, rows, turn, orders : 2 * orders] = -np.sin(angle)
        table[:, 1, rows, turn, :orders] = np.sin(angle)
        table[:, 1, rows, turn, orders : 2 * orders] = np.cos(angle)
    return table.reshape(blks * 2 * lines, turns * groups)


def exchange_kernel(turns, lines, sums_ref, table_ref, order_ref, all_ref, from_ref, *scratch):
    recv, out, sum_send, sum_recv, all_send, all_recv = scratch
    ells, blks = lax.axis_size("ell"), lax.axis_size("blk")
    ell, blk = lax.axis_index("ell"), lax.axis_index("blk")
    pieces, _, width = sums_ref.shape
    rows = recv.shape[2]
    block = 2 * lines

    barrier = pltpu.get_barrier_semaphore()
    for step in range(1, ells):
        pl.semaphore_signal(barrier, inc=1, device_id={"ell": lax.rem(ell + step, ells)}, device_id_type=MESH)
    for step in range(1, blks):
        pl.semaphore_signal(barrier, inc=1, device_id={"blk": lax.rem(blk + step, blks)}, device_id_type=MESH)
    pl.semaphore_wait(barrier, ells + blks - 2)

    def sum_copy(piece, step):
        target = lax.rem(ell + step, ells)
        return pltpu.make_async_remote_copy(
            src_ref=sums_ref.at[piece, pl.ds(pl.multiple_of(target * rows, SUBLANES), rows), :],
            dst_ref=recv.at[step - 1, piece],
            send_sem=sum_send.at[piece, step - 1],
            recv_sem=sum_recv.at[piece, step - 1],
            device_id={"ell": target},
            device_id_type=MESH,
        )

    def all_copy(piece, step):
        target = lax.rem(blk + step, blks)
        return pltpu.make_async_remote_copy(
            src_ref=out.at[piece, pl.ds(pl.multiple_of(target * block, SUBLANES), block), :],
            dst_ref=all_ref.at[blk, piece],
            send_sem=all_send.at[piece, step - 1],
            recv_sem=all_recv.at[piece, step - 1],
            device_id={"blk": target},
            device_id_type=MESH,
        )

    for piece in range(pieces):
        for step in range(1, ells):
            sum_copy(piece, step).start()

    order = order_ref[...]
    total = order.shape[1]
    first = from_ref.shape[0] * 2
    span = total // first
    place = (order % first) // 2
    lane = (order % 2) * span + order // first
    column = lax.broadcasted_iota(jnp.int32, (from_ref.shape[0], total), 1)
    here = lax.broadcasted_iota(jnp.int32, (from_ref.shape[0], total), 0) == place
    pick = lambda x: jnp.where(here, x, 0).astype(jnp.float32).astype(jnp.bfloat16)
    left = jnp.concatenate([pick(column // 16), pick(column % 16)], axis=0)
    right = lax.broadcasted_iota(jnp.int32, (LANES, total), 0) == lane
    right = right.astype(jnp.float32).astype(jnp.bfloat16)
    found = lax.dot_general(left, right, (((1,), (1,)), ((), ())), preferred_element_type=jnp.float32)
    half = from_ref.shape[0]
    from_ref[...] = (found[:half] * 16.0 + found[half:]).astype(jnp.int32)

    table = (table_ref[0], table_ref[1])
    for piece in range(pieces):
        total = sums_ref[piece, pl.ds(pl.multiple_of(ell * rows, SUBLANES), rows), :]
        for step in range(1, ells):
            sum_copy(piece, step).wait_recv()
            total = total + recv[step - 1, piece]
        out[piece] = product(table, split(total))
        for step in range(1, blks):
            all_copy(piece, step).start()
        all_ref[blk, piece] = out[piece, pl.ds(pl.multiple_of(blk * block, SUBLANES), block), :]

    for piece in range(pieces):
        for step in range(1, blks):
            all_copy(piece, step).wait_recv()
    for piece in range(pieces):
        for step in range(1, ells):
            sum_copy(piece, step).wait_send()
        for step in range(1, blks):
            all_copy(piece, step).wait_send()


def exchange(sums, order_of_column, orders, cycles):
    ells, blks = lax.axis_size("ell"), lax.axis_size("blk")
    pieces, _, width = sums.shape
    turns, samples = cycles // ells, NPSI // blks
    lines = round_up(turns * samples, SUBLANES)
    rows = turns * round_up(2 * orders, SUBLANES)
    total = order_of_column.shape[0]
    table = split_table(psi_rows(orders, blks, turns, samples))
    in_vmem = pl.BlockSpec(memory_space=pltpu.VMEM)
    return pl.pallas_call(
        functools.partial(exchange_kernel, turns, lines),
        out_shape=(
            jax.ShapeDtypeStruct((blks, pieces, 2 * lines, width), jnp.float32),
            jax.ShapeDtypeStruct((total // LANES, LANES), jnp.int32),
        ),
        in_specs=[in_vmem] * 3,
        out_specs=(in_vmem, in_vmem),
        scratch_shapes=[
            pltpu.VMEM((ells - 1, pieces, rows, width), jnp.float32),
            pltpu.VMEM((pieces, blks * 2 * lines, width), jnp.float32),
            pltpu.SemaphoreType.DMA((pieces, ells - 1)),
            pltpu.SemaphoreType.DMA((pieces, ells - 1)),
            pltpu.SemaphoreType.DMA((pieces, blks - 1)),
            pltpu.SemaphoreType.DMA((pieces, blks - 1)),
        ],
        compiler_params=pltpu.CompilerParams(
            collective_id=0, has_side_effects=True, vmem_limit_bytes=32 * 1024 * 1024
        ),
        name="exchange",
    )(sums, table, order_of_column[None, :])


def turned(value, turn, period):
    real, imag = value
    turn = turn % period
    if turn == 0:
        return real, imag
    if 4 * turn == period:
        return -imag, real
    cos, sin = math.cos(2.0 * math.pi * turn / period), math.sin(2.0 * math.pi * turn / period)
    return real * cos - imag * sin, real * sin + imag * cos


def transform(values):
    size = len(values)
    if size == 1:
        return values
    even, odd = transform(values[0::2]), transform(values[1::2])
    odd = [turned(value, j, size) for j, value in enumerate(odd)]
    low = [(e[0] + o[0], e[1] + o[1]) for e, o in zip(even, odd)]
    high = [(e[0] - o[0], e[1] - o[1]) for e, o in zip(even, odd)]
    return low + high


def phi_kernel(lines, all_ref, from_ref, table_ref, twist_ref, out_ref):
    turns, samples, _ = out_ref.shape
    blks, pieces, _, width = all_ref.shape
    places = from_ref.shape[0]
    per = LANES // width
    real, imag = [], []
    blocks = [(b, piece) for b in range(blks) for piece in range(pieces)]
    for tile in range(len(blocks) // per):
        for rows, into in ((pl.ds(0, lines), real), (pl.ds(lines, lines), imag)):
            part = [all_ref[b, piece, rows, :] for b, piece in blocks[tile * per : (tile + 1) * per]]
            into.append(part[0] if per == 1 else jnp.concatenate(part, axis=1))
    rows = []
    for place in range(places):
        source = jnp.broadcast_to(from_ref[pl.ds(place, 1), :], (lines, LANES))
        high, index = source >> 7, source & (LANES - 1)
        both = []
        for tiles in (real, imag):
            picked = lane_pick(tiles[0], index)
            for t in range(1, len(tiles)):
                picked = jnp.where(high == t, lane_pick(tiles[t], index), picked)
            both.append(picked)
        rows.append(jnp.concatenate(both, axis=1))
    first = product(split(jnp.concatenate(rows, axis=0)), (table_ref[0], table_ref[1]))
    values = []
    for place in range(places):
        here = first[place * lines : (place + 1) * lines]
        for side in range(2):
            re = here[:, 2 * side * LANES : (2 * side + 1) * LANES]
            im = here[:, (2 * side + 1) * LANES : (2 * side + 2) * LANES]
            cos = jnp.broadcast_to(twist_ref[0, pl.ds(2 * place + side, 1), :], (lines, LANES))
            sin = jnp.broadcast_to(twist_ref[1, pl.ds(2 * place + side, 1), :], (lines, LANES))
            values.append((re * cos - im * sin, re * sin + im * cos))
    for j, (value, _) in enumerate(transform(values)):
        for turn in range(turns):
            out_ref[turn, :, j * LANES : (j + 1) * LANES] = value[turn * samples : (turn + 1) * samples]


def phi_tables(degrees):
    outer = 2 * degrees // LANES
    span = degrees // outer
    angle = 2.0 * np.pi * np.outer(np.arange(span), np.arange(LANES)) / LANES
    table = np.zeros((2, 2, span, 2, 2, LANES))
    for side in range(2):
        table[0, side, :, side, 0] = np.cos(angle)
        table[0, side, :, side, 1] = np.sin(angle)
        table[1, side, :, side, 0] = -np.sin(angle)
        table[1, side, :, side, 1] = np.cos(angle)
    angle = 2.0 * np.pi * np.outer(np.arange(outer), np.arange(LANES)) / (2 * degrees)
    return table.reshape(4 * span, 4 * LANES), np.stack([np.cos(angle), np.sin(angle)])


def to_phi(gathered, origin, turns, samples, degrees):
    table, twist = phi_tables(degrees)
    in_vmem = pl.BlockSpec(memory_space=pltpu.VMEM)
    return pl.pallas_call(
        functools.partial(phi_kernel, gathered.shape[2] // 2),
        out_shape=jax.ShapeDtypeStruct((turns, samples, 2 * degrees), jnp.float32),
        in_specs=[in_vmem] * 4,
        out_specs=in_vmem,
        compiler_params=pltpu.CompilerParams(vmem_limit_bytes=32 * 1024 * 1024),
        name="to_phi",
    )(gathered, origin, split_table(table), jnp.asarray(twist, jnp.float32))


def on_device(wigner, sky_alm, beam_blm, slot_col, slot_ell, order_of_column):
    cycles, orders, _ = wigner.shape
    degrees = order_of_column.shape[0]
    ells, blks = lax.axis_size("ell"), lax.axis_size("blk")
    sums = order_sums(wigner, sky_alm, beam_blm, slot_col, slot_ell, degrees // blks)
    gathered, origin = exchange(sums, order_of_column, orders, cycles)
    return to_phi(gathered, origin, cycles // ells, NPSI // blks, degrees)


def solution(mesh):
    return jax.shard_map(
        on_device,
        mesh=mesh,
        in_specs=(
            P(None, None, ("ell", "blk")),
            P(None, ("ell", "blk")),
            P(),
            P(("ell", "blk")),
            P(("ell", "blk")),
            P(),
        ),
        out_specs=P("ell", "blk", None),
        check_vma=False,
    )
```

```python
import functools
import math

import jax
import jax.numpy as jnp
import numpy as np
from jax import lax
from jax.experimental import pallas as pl
from jax.experimental.pallas import tpu as pltpu
from jax.sharding import PartitionSpec as P

NPSI = 32
LANES = 128
SUBLANES = 8
MXU = 256
MXU_ROWS = 1024
TRIP = 16
MESH = pl.DeviceIdType.MESH


def round_up(value, step):
    return -(-value // step) * step


def lane_pick(table, index):
    return lax.gather(
        table,
        index[..., None],
        lax.GatherDimensionNumbers(
            offset_dims=(),
            collapsed_slice_dims=(1,),
            start_index_map=(1,),
            operand_batching_dims=(0,),
            start_indices_batching_dims=(0,),
        ),
        slice_sizes=(1, 1),
        mode=lax.GatherScatterMode.PROMISE_IN_BOUNDS,
    )


REAL_STEP = 1 << 19
IMAG_SHIFT = 13
POWER_BITS = 6
LEAST_POWER = 62
FULL = 4094.0


def largest(blocks):
    most = functools.reduce(jnp.maximum, [jnp.abs(block) for block in blocks])
    return jnp.max(most, axis=(0, 1), keepdims=True)


def pack_beam(real_ref, imag_ref, table_ref):
    orders, degrees = table_ref.shape
    most = jnp.maximum(largest([real_ref[...], imag_ref[...]]), 1e-30)
    unit = jnp.broadcast_to(1.0 / most, (orders, LANES))
    for tile in range(degrees // LANES):
        lanes = pl.ds(tile * LANES, LANES)
        real, imag = real_ref[:, lanes] * unit, imag_ref[:, lanes] * unit
        size = jnp.maximum(jnp.abs(real), jnp.abs(imag))
        power = jnp.floor(jnp.log2(size)) + 1.0
        power = jnp.minimum(jnp.maximum(power, -float(LEAST_POWER)), 1.0)
        grow = jnp.exp2(-power) * FULL
        code = (power + float(LEAST_POWER)).astype(jnp.int32)
        below = code.astype(jnp.float32) * (1.0 / 64.0)
        imag_code = jnp.floor(imag * grow - below + 0.5).astype(jnp.int32)
        low = ((imag_code & 0x1FFF) << POWER_BITS) + code
        below = low.astype(jnp.float32) * (1.0 / REAL_STEP)
        real_code = jnp.floor(real * grow - below + 0.5).astype(jnp.int32)
        table_ref[:, lanes] = (real_code << 19) + low
    return most


def pick_span(col_ref, ell_ref, tiles):
    live = col_ref[...] >= 0
    degree = ell_ref[...]
    last = tiles * LANES - 1
    top = jnp.max(jnp.where(live, degree, 0).astype(jnp.float32)).astype(jnp.int32)
    low = jnp.min(jnp.where(live, degree, last).astype(jnp.float32)).astype(jnp.int32)
    return low // LANES, top // LANES


def sums_kernel(orders, cols, trips, groups, wig_hbm, sky_hbm, col_hbm, ell_hbm, beam_hbm, out_ref, *scratch):
    wig_buf, tail_buf, sky_ref, col_ref, ell_ref, real_ref, imag_ref, table_ref = scratch[0:8]
    coeff_refs, sems, once = scratch[8:12], scratch[12], scratch[13]
    cycles = wig_hbm.shape[1]
    tiles = table_ref.shape[1] // LANES
    slot_tiles = col_ref.shape[0]
    rest = slot_tiles - trips * TRIP
    depth = wig_buf.shape[0]
    half = orders * cycles
    by_rows = 2 * half > MXU_ROWS

    def wig_copy(trip, slot):
        lanes = pl.ds(pl.multiple_of(trip * (TRIP * LANES), LANES), TRIP * LANES)
        return pltpu.make_async_copy(wig_hbm.at[:, :, lanes], wig_buf.at[slot], sems.at[slot])

    rest_lanes = pl.ds(trips * TRIP * LANES, rest * LANES)
    ell_copy = pltpu.make_async_copy(ell_hbm, ell_ref, once.at[0])
    col_copy = pltpu.make_async_copy(col_hbm, col_ref, once.at[1])
    real_copy = pltpu.make_async_copy(beam_hbm.at[:, 0, :], real_ref, once.at[2])
    imag_copy = pltpu.make_async_copy(beam_hbm.at[:, 1, :], imag_ref, once.at[3])
    sky_copy = pltpu.make_async_copy(sky_hbm, sky_ref, once.at[4])
    for copy in (real_copy, imag_copy, col_copy, ell_copy, sky_copy):
        copy.start()
    for trip in range(min(depth - 2, trips)):
        wig_copy(trip, trip).start()
    if rest:
        tail_copy = pltpu.make_async_copy(wig_hbm.at[:, :, rest_lanes], tail_buf, once.at[5])
        tail_copy.start()

    real_copy.wait()
    imag_copy.wait()
    most = pack_beam(real_ref, imag_ref, table_ref)
    unit = jnp.broadcast_to(most * (1.0 / (REAL_STEP * FULL)), (SUBLANES, LANES))
    col_copy.wait()
    ell_copy.wait()
    low, top = pick_span(col_ref, ell_ref, tiles)
    span = top - low + 1
    sky_copy.wait()
    row16 = lax.broadcasted_iota(jnp.int32, (16, LANES), 0).astype(jnp.float32).astype(jnp.bfloat16)

    def coeffs(count, first, tile, rows, coeff):
        degree = ell_ref[pl.ds(tile, rows), :]
        lanes = pl.ds(pl.multiple_of(tile * LANES, LANES), rows * LANES)
        sky_re = sky_ref[pl.ds(0, 1), lanes].reshape(rows, LANES) * unit[:rows]
        sky_im = sky_ref[pl.ds(1, 1), lanes].reshape(rows, LANES) * unit[:rows]
        high = (degree >> 7) - first
        index = degree & (LANES - 1)
        here = [high == t for t in range(1, count)]
        for order in range(orders):
            word = None
            for t in range(count):
                lanes = pl.ds(pl.multiple_of((first + t) * LANES, LANES), LANES)
                entry = jnp.broadcast_to(table_ref[pl.ds(order, 1), lanes], (rows, LANES))
                value = lane_pick(entry, index)
                word = value if t == 0 else jnp.where(here[t - 1], value, word)
            real = word.astype(jnp.float32)
            imag = (word << IMAG_SHIFT).astype(jnp.float32)
            power = jnp.exp2((word & (2**POWER_BITS - 1)).astype(jnp.float32) - float(LEAST_POWER))
            real, imag = real * power, imag * power
            coeff[order, pl.ds(0, rows), :] = sky_re * real - sky_im * imag
            coeff[orders + order, pl.ds(0, rows), :] = sky_re * imag + sky_im * real

    def values(wig, coeff, part, start, line):
        out = []
        for order in range(orders):
            here = wig[order, :, pl.ds(start, LANES)].astype(jnp.float32)
            row = coeff[part * orders + order, pl.ds(line, 1), :]
            out.append(here * jnp.broadcast_to(row, (cycles, LANES)))
        return jnp.concatenate(out, axis=0)

    def hot(tile):
        line = jnp.broadcast_to(col_ref[pl.ds(tile, 1), :], (16, LANES))
        away = line.astype(jnp.float32).astype(jnp.bfloat16) - row16
        one, zero = jnp.ones_like(away), jnp.zeros_like(away)
        out = [jnp.where(away == jnp.bfloat16(16 * g), one, zero) for g in range(cols // 16)]
        out += [zero] * (MXU // 16 - cols // 16)
        return jnp.concatenate(out, axis=0)

    def body(acc0, acc1):
        accs = (acc0, acc1)
        if by_rows:
            work = lambda i: [(0, i % 2, (0,)), (1, i % 2, (1,))]
        else:
            work = lambda i: [(i % 2, i // 2 % 2, (0, 1))]

        ahead = 2 if by_rows else 4

        def push(i, tile, count=2):
            left = hot(tile)
            right = hot(tile + 1) if count == 2 else jnp.zeros_like(left)
            both = jnp.concatenate([left, right], axis=1)
            for mxu, register, _ in work(i):
                pltpu.matmul_push_rhs(both, register, mxu, transpose=True)

        def multiply(i, wig, coeff, start, line, count=2):
            for mxu, register, parts in work(i):
                blocks = []
                for part in parts:
                    left = values(wig, coeff, part, start, line)
                    if count == 2:
                        right = values(wig, coeff, part, start + LANES, line + 1)
                    else:
                        right = jnp.zeros_like(left)
                    blocks.append(jnp.concatenate([left, right], axis=1))
                block = blocks[0] if len(blocks) == 1 else jnp.concatenate(blocks, axis=0)
                pltpu.matmul_acc_lhs(accs[mxu], block, load_staged_rhs=register)

        pairs = TRIP // 2
        tail_pairs = -(-rest // 2)

        def tail_size(i):
            return min(2, rest - 2 * i)

        def run(count, first):
            for which in range(TRIP // SUBLANES):
                coeffs(count, first, which * SUBLANES, SUBLANES, coeff_refs[which])
            for i in range(ahead):
                push(i, 2 * i)

            def trip_body(trip, turn, last):
                wig = wig_buf.at[lax.rem(trip, depth)]
                base = trip * TRIP
                now, later = coeff_refs[2 * turn : 2 * turn + 2], coeff_refs[2 - 2 * turn : 4 - 2 * turn]
                for i in range(pairs):
                    which = 2 * i // SUBLANES
                    if 2 * i % SUBLANES == 0:
                        lines = min(max(rest - which * SUBLANES, 0), SUBLANES) if last else SUBLANES
                        tile = base + TRIP + which * SUBLANES
                        if not last:
                            tile = pl.multiple_of(tile, SUBLANES)
                        if lines:
                            coeffs(count, first, tile, lines, later[which])
                    multiply(i, wig, now[which], 2 * i * LANES, 2 * i % SUBLANES)
                    after = i + ahead
                    if not last or after < pairs:
                        push(after, base + 2 * after)
                    elif after - pairs < tail_pairs:
                        push(after, base + 2 * after, tail_size(after - pairs))

            def arrived(trip):
                wig_copy(trip, lax.rem(trip, depth)).wait()

            def ask(trip):
                @pl.when(trip < trips)
                def _():
                    wig_copy(trip, lax.rem(trip, depth)).start()

            turns = (trips - 1) // 2
            if turns:

                @pl.loop(0, turns)
                def _(turn):
                    ask(2 * turn + depth - 2)
                    ask(2 * turn + depth - 1)
                    arrived(2 * turn)
                    arrived(2 * turn + 1)
                    trip_body(2 * turn, 0, False)
                    trip_body(2 * turn + 1, 1, False)

            for trip in range(2 * turns, trips):
                arrived(trip)
            if rest:
                tail_copy.wait()
            for trip in range(2 * turns, trips):
                trip_body(trip, trip % 2, trip == trips - 1)
            later = coeff_refs[2:4] if trips % 2 else coeff_refs[0:2]
            for i in range(tail_pairs):
                multiply(pairs + i, tail_buf, later[2 * i // SUBLANES], 2 * i * LANES, 2 * i % SUBLANES, tail_size(i))
                if ahead + i < tail_pairs:
                    tile = trips * TRIP + 2 * (i + ahead)
                    push(pairs + i + ahead, tile, tail_size(i + ahead))

        counts = sorted({min(c, tiles) for c in (4, 9)})
        below = 0
        for count in counts:
            first = jnp.minimum(low, tiles - count)

            @pl.when((span > below) & (span <= count) if below else span <= count)
            def _():
                run(count, first)

            below = count
        if below < tiles:

            @pl.when(span > below)
            def _():
                run(tiles, 0)

        width = out_ref.shape[2]
        sums = [pltpu.matmul_pop(acc0), pltpu.matmul_pop(acc1)]
        if not by_rows:
            sums = [sums[0] + sums[1]]
        sums = jnp.concatenate(sums, axis=0)
        for piece in range(cols // width):
            lanes = slice(piece * width, (piece + 1) * width)
            for cycle in range(cycles):
                if groups > 2 * orders:
                    pad = pl.ds(cycle * groups + 2 * orders, groups - 2 * orders)
                    out_ref[piece, pad, :] = jnp.zeros((groups - 2 * orders, width), jnp.float32)
            for row in range(2 * orders):
                for cycle in range(0, cycles, SUBLANES):
                    here = pl.ds(cycle * groups + row, SUBLANES, stride=groups)
                    start = row * cycles + cycle
                    out_ref[piece, here, :] = sums[start : start + SUBLANES, lanes]

    rows = half if by_rows else 2 * half
    pl.run_scoped(body, pltpu.ACC(0)((rows, MXU), jnp.float32), pltpu.ACC(1)((rows, MXU), jnp.float32))


def order_sums(wigner, sky_alm, beam_blm, slot_col, slot_ell, cols, groups):
    cycles, orders, slots = wigner.shape
    degrees = beam_blm.shape[2]
    tiles = slots // LANES
    trips = tiles // TRIP
    rest = tiles - trips * TRIP
    depth = 8
    width = min(cols, LANES)
    shape = (cols // width, cycles * groups, width)
    in_hbm = lambda x: pltpu.with_memory_space_constraint(x, pltpu.HBM)
    return pl.pallas_call(
        functools.partial(sums_kernel, orders, cols, trips, groups),
        out_shape=jax.ShapeDtypeStruct(shape, jnp.float32),
        in_specs=[pl.BlockSpec(memory_space=pltpu.HBM)] * 5,
        out_specs=pl.BlockSpec(memory_space=pltpu.VMEM),
        scratch_shapes=[
            pltpu.VMEM((depth, orders, cycles, TRIP * LANES), jnp.bfloat16),
            pltpu.VMEM((orders, cycles, max(rest, 1) * LANES), jnp.bfloat16),
            pltpu.VMEM((2, slots), jnp.float32),
            pltpu.VMEM((tiles, LANES), jnp.int32),
            pltpu.VMEM((tiles, LANES), jnp.int32),
            pltpu.VMEM((orders, degrees), jnp.float32),
            pltpu.VMEM((orders, degrees), jnp.float32),
            pltpu.VMEM((orders, degrees), jnp.int32),
            *[pltpu.VMEM((2 * orders, SUBLANES, LANES), jnp.float32) for _ in range(4)],
            pltpu.SemaphoreType.DMA((depth,)),
            pltpu.SemaphoreType.DMA((6,)),
        ],
        compiler_params=pltpu.CompilerParams(vmem_limit_bytes=32 * 1024 * 1024),
        name="order_sums",
    )(
        in_hbm(wigner.transpose(1, 0, 2)),
        in_hbm(sky_alm),
        in_hbm(slot_col.reshape(tiles, LANES)),
        in_hbm(slot_ell.reshape(tiles, LANES)),
        in_hbm(beam_blm.transpose(1, 0, 2)),
    )


def split(value):
    high = value.astype(jnp.bfloat16)
    return high, (value - high.astype(jnp.float32)).astype(jnp.bfloat16)


def split_table(table):
    high, low = split(jnp.asarray(table, jnp.float32))
    return jnp.stack([high, low])


def product(left, right):
    dot = functools.partial(jnp.dot, preferred_element_type=jnp.float32)
    return dot(left[0], right[0]) + dot(left[0], right[1]) + dot(left[1], right[0])


def line_step(orders, turns):
    step = 2 * orders
    while turns * step % SUBLANES:
        step += 1
    return step


def psi_rows(orders, blks, turns, samples):
    groups, lines = line_step(orders, turns), round_up(turns * samples, SUBLANES)
    table = np.zeros((blks, 2, lines, turns, groups))
    sample = np.arange(blks * samples).reshape(blks, samples)
    angle = 2.0 * np.pi * (sample[..., None] * np.arange(orders) % (blks * samples)) / (blks * samples)
    for turn in range(turns):
        rows = slice(turn * samples, (turn + 1) * samples)
        table[:, 0, rows, turn, :orders] = np.cos(angle)
        table[:, 0, rows, turn, orders : 2 * orders] = -np.sin(angle)
        table[:, 1, rows, turn, :orders] = np.sin(angle)
        table[:, 1, rows, turn, orders : 2 * orders] = np.cos(angle)
    return table.reshape(blks * 2 * lines, turns * groups)


def exchange_kernel(turns, lines, sums_ref, table_ref, order_ref, all_ref, from_ref, *scratch):
    recv, out, sum_send, sum_recv, all_send, all_recv = scratch
    ells, blks = lax.axis_size("ell"), lax.axis_size("blk")
    ell, blk = lax.axis_index("ell"), lax.axis_index("blk")
    pieces, _, width = sums_ref.shape
    rows = recv.shape[2]
    block = 2 * lines

    barrier = pltpu.get_barrier_semaphore()
    for step in range(1, ells):
        pl.semaphore_signal(barrier, inc=1, device_id={"ell": lax.rem(ell + step, ells)}, device_id_type=MESH)
    for step in range(1, blks):
        pl.semaphore_signal(barrier, inc=1, device_id={"blk": lax.rem(blk + step, blks)}, device_id_type=MESH)
    pl.semaphore_wait(barrier, ells + blks - 2)

    def sum_copy(piece, step):
        target = lax.rem(ell + step, ells)
        return pltpu.make_async_remote_copy(
            src_ref=sums_ref.at[piece, pl.ds(pl.multiple_of(target * rows, SUBLANES), rows), :],
            dst_ref=recv.at[step - 1, piece],
            send_sem=sum_send.at[piece, step - 1],
            recv_sem=sum_recv.at[piece, step - 1],
            device_id={"ell": target},
            device_id_type=MESH,
        )

    def all_copy(piece, step):
        target = lax.rem(blk + step, blks)
        return pltpu.make_async_remote_copy(
            src_ref=out.at[piece, pl.ds(pl.multiple_of(target * block, SUBLANES), block), :],
            dst_ref=all_ref.at[blk, piece],
            send_sem=all_send.at[piece, step - 1],
            recv_sem=all_recv.at[piece, step - 1],
            device_id={"blk": target},
            device_id_type=MESH,
        )

    for piece in range(pieces):
        for step in range(1, ells):
            sum_copy(piece, step).start()

    order = order_ref[...]
    total = order.shape[1]
    first = from_ref.shape[0] * 2
    span = total // first
    place = (order % first) // 2
    lane = (order % 2) * span + order // first
    column = lax.broadcasted_iota(jnp.int32, (from_ref.shape[0], total), 1)
    here = lax.broadcasted_iota(jnp.int32, (from_ref.shape[0], total), 0) == place
    pick = lambda x: jnp.where(here, x, 0).astype(jnp.float32).astype(jnp.bfloat16)
    left = jnp.concatenate([pick(column // 16), pick(column % 16)], axis=0)
    right = lax.broadcasted_iota(jnp.int32, (LANES, total), 0) == lane
    right = right.astype(jnp.float32).astype(jnp.bfloat16)
    found = lax.dot_general(left, right, (((1,), (1,)), ((), ())), preferred_element_type=jnp.float32)
    half = from_ref.shape[0]
    from_ref[...] = (found[:half] * 16.0 + found[half:]).astype(jnp.int32)

    table = (table_ref[0], table_ref[1])
    for piece in range(pieces):
        total = sums_ref[piece, pl.ds(pl.multiple_of(ell * rows, SUBLANES), rows), :]
        for step in range(1, ells):
            sum_copy(piece, step).wait_recv()
            total = total + recv[step - 1, piece]
        out[piece] = product(table, split(total))
        for step in range(1, blks):
            all_copy(piece, step).start()
        all_ref[blk, piece] = out[piece, pl.ds(pl.multiple_of(blk * block, SUBLANES), block), :]

    for piece in range(pieces):
        for step in range(1, blks):
            all_copy(piece, step).wait_recv()
    for piece in range(pieces):
        for step in range(1, ells):
            sum_copy(piece, step).wait_send()
        for step in range(1, blks):
            all_copy(piece, step).wait_send()


def exchange(sums, order_of_column, orders, cycles):
    ells, blks = lax.axis_size("ell"), lax.axis_size("blk")
    pieces, _, width = sums.shape
    turns, samples = cycles // ells, NPSI // blks
    lines = round_up(turns * samples, SUBLANES)
    rows = turns * line_step(orders, turns)
    total = order_of_column.shape[0]
    table = split_table(psi_rows(orders, blks, turns, samples))
    in_vmem = pl.BlockSpec(memory_space=pltpu.VMEM)
    return pl.pallas_call(
        functools.partial(exchange_kernel, turns, lines),
        out_shape=(
            jax.ShapeDtypeStruct((blks, pieces, 2 * lines, width), jnp.float32),
            jax.ShapeDtypeStruct((total // LANES, LANES), jnp.int32),
        ),
        in_specs=[in_vmem] * 3,
        out_specs=(in_vmem, in_vmem),
        scratch_shapes=[
            pltpu.VMEM((ells - 1, pieces, rows, width), jnp.float32),
            pltpu.VMEM((pieces, blks * 2 * lines, width), jnp.float32),
            pltpu.SemaphoreType.DMA((pieces, ells - 1)),
            pltpu.SemaphoreType.DMA((pieces, ells - 1)),
            pltpu.SemaphoreType.DMA((pieces, blks - 1)),
            pltpu.SemaphoreType.DMA((pieces, blks - 1)),
        ],
        compiler_params=pltpu.CompilerParams(
            collective_id=0, has_side_effects=True, vmem_limit_bytes=32 * 1024 * 1024
        ),
        name="exchange",
    )(sums, table, order_of_column[None, :])


def turned(value, turn, period):
    real, imag = value
    turn = turn % period
    if turn == 0:
        return real, imag
    if 4 * turn == period:
        return -imag, real
    cos, sin = math.cos(2.0 * math.pi * turn / period), math.sin(2.0 * math.pi * turn / period)
    return real * cos - imag * sin, real * sin + imag * cos


def transform(values):
    size = len(values)
    if size == 1:
        return values
    even, odd = transform(values[0::2]), transform(values[1::2])
    odd = [turned(value, j, size) for j, value in enumerate(odd)]
    low = [(e[0] + o[0], e[1] + o[1]) for e, o in zip(even, odd)]
    high = [(e[0] - o[0], e[1] - o[1]) for e, o in zip(even, odd)]
    return low + high


def phi_kernel(lines, all_ref, from_ref, table_ref, twist_ref, out_ref):
    turns, samples, _ = out_ref.shape
    blks, pieces, _, width = all_ref.shape
    places = from_ref.shape[0]
    per = LANES // width
    real, imag = [], []
    blocks = [(b, piece) for b in range(blks) for piece in range(pieces)]
    for tile in range(len(blocks) // per):
        for rows, into in ((pl.ds(0, lines), real), (pl.ds(lines, lines), imag)):
            part = [all_ref[b, piece, rows, :] for b, piece in blocks[tile * per : (tile + 1) * per]]
            into.append(part[0] if per == 1 else jnp.concatenate(part, axis=1))
    rows = []
    for place in range(places):
        source = jnp.broadcast_to(from_ref[pl.ds(place, 1), :], (lines, LANES))
        high, index = source >> 7, source & (LANES - 1)
        both = []
        for tiles in (real, imag):
            picked = lane_pick(tiles[0], index)
            for t in range(1, len(tiles)):
                picked = jnp.where(high == t, lane_pick(tiles[t], index), picked)
            both.append(picked)
        rows.append(jnp.concatenate(both, axis=1))
    first = product(split(jnp.concatenate(rows, axis=0)), (table_ref[0], table_ref[1]))
    values = []
    for place in range(places):
        here = first[place * lines : (place + 1) * lines]
        for side in range(2):
            re = here[:, 2 * side * LANES : (2 * side + 1) * LANES]
            im = here[:, (2 * side + 1) * LANES : (2 * side + 2) * LANES]
            cos = jnp.broadcast_to(twist_ref[0, pl.ds(2 * place + side, 1), :], (lines, LANES))
            sin = jnp.broadcast_to(twist_ref[1, pl.ds(2 * place + side, 1), :], (lines, LANES))
            values.append((re * cos - im * sin, re * sin + im * cos))
    for j, (value, _) in enumerate(transform(values)):
        for turn in range(turns):
            out_ref[turn, :, j * LANES : (j + 1) * LANES] = value[turn * samples : (turn + 1) * samples]


def phi_tables(degrees):
    outer = 2 * degrees // LANES
    span = degrees // outer
    angle = 2.0 * np.pi * np.outer(np.arange(span), np.arange(LANES)) / LANES
    table = np.zeros((2, 2, span, 2, 2, LANES))
    for side in range(2):
        table[0, side, :, side, 0] = np.cos(angle)
        table[0, side, :, side, 1] = np.sin(angle)
        table[1, side, :, side, 0] = -np.sin(angle)
        table[1, side, :, side, 1] = np.cos(angle)
    angle = 2.0 * np.pi * np.outer(np.arange(outer), np.arange(LANES)) / (2 * degrees)
    return table.reshape(4 * span, 4 * LANES), np.stack([np.cos(angle), np.sin(angle)])


def to_phi(gathered, origin, turns, samples, degrees):
    table, twist = phi_tables(degrees)
    in_vmem = pl.BlockSpec(memory_space=pltpu.VMEM)
    return pl.pallas_call(
        functools.partial(phi_kernel, gathered.shape[2] // 2),
        out_shape=jax.ShapeDtypeStruct((turns, samples, 2 * degrees), jnp.float32),
        in_specs=[in_vmem] * 4,
        out_specs=in_vmem,
        compiler_params=pltpu.CompilerParams(vmem_limit_bytes=32 * 1024 * 1024),
        name="to_phi",
    )(gathered, origin, split_table(table), jnp.asarray(twist, jnp.float32))


def on_device(wigner, sky_alm, beam_blm, slot_col, slot_ell, order_of_column):
    cycles, orders, _ = wigner.shape
    degrees = order_of_column.shape[0]
    ells, blks = lax.axis_size("ell"), lax.axis_size("blk")
    sums = order_sums(wigner, sky_alm, beam_blm, slot_col, slot_ell, degrees // blks, line_step(orders, cycles // ells))
    gathered, origin = exchange(sums, order_of_column, orders, cycles)
    return to_phi(gathered, origin, cycles // ells, NPSI // blks, degrees)


def solution(mesh):
    return jax.shard_map(
        on_device,
        mesh=mesh,
        in_specs=(
            P(None, None, ("ell", "blk")),
            P(None, ("ell", "blk")),
            P(),
            P(("ell", "blk")),
            P(("ell", "blk")),
            P(),
        ),
        out_specs=P("ell", "blk", None),
        check_vma=False,
    )
```

```python
import functools
import math

import jax
import jax.numpy as jnp
import numpy as np
from jax import lax
from jax.experimental import pallas as pl
from jax.experimental.pallas import tpu as pltpu
from jax.sharding import PartitionSpec as P

NPSI = 32
LANES = 128
SUBLANES = 8
MXU = 256
MXU_ROWS = 1024
TRIP = 16
MESH = pl.DeviceIdType.MESH


def round_up(value, step):
    return -(-value // step) * step


def lane_pick(table, index):
    return lax.gather(
        table,
        index[..., None],
        lax.GatherDimensionNumbers(
            offset_dims=(),
            collapsed_slice_dims=(1,),
            start_index_map=(1,),
            operand_batching_dims=(0,),
            start_indices_batching_dims=(0,),
        ),
        slice_sizes=(1, 1),
        mode=lax.GatherScatterMode.PROMISE_IN_BOUNDS,
    )


REAL_BITS = 19
IMAG_SHIFT = 13
POWER_BITS = 6
LEAST_POWER = 62
FULL = 4094.0


def largest(blocks):
    most = functools.reduce(jnp.maximum, [jnp.abs(block) for block in blocks])
    return jnp.max(most, axis=(0, 1), keepdims=True)


def pack_beam(real_ref, imag_ref, table_ref):
    orders, degrees = table_ref.shape
    most = jnp.maximum(largest([real_ref[...], imag_ref[...]]), 1e-30)
    unit = jnp.broadcast_to(1.0 / most, (orders, LANES))
    for tile in range(degrees // LANES):
        lanes = pl.ds(tile * LANES, LANES)
        real, imag = real_ref[:, lanes] * unit, imag_ref[:, lanes] * unit
        size = jnp.maximum(jnp.abs(real), jnp.abs(imag))
        power = jnp.floor(jnp.log2(size)) + 1.0
        power = jnp.minimum(jnp.maximum(power, -float(LEAST_POWER)), 1.0)
        grow = jnp.exp2(-power) * FULL
        code = (power + float(LEAST_POWER)).astype(jnp.int32)
        below = code.astype(jnp.float32) * (1.0 / 64.0)
        imag_code = jnp.floor(imag * grow - below + 0.5).astype(jnp.int32)
        low = ((imag_code & 0x1FFF) << POWER_BITS) + code
        below = low.astype(jnp.float32) * (1.0 / 2**REAL_BITS)
        real_code = jnp.floor(real * grow - below + 0.5).astype(jnp.int32)
        table_ref[:, lanes] = (real_code << REAL_BITS) + low
    return most


def pick_span(col_ref, ell_ref, tiles):
    live = col_ref[...] >= 0
    degree = ell_ref[...]
    last = tiles * LANES - 1
    top = jnp.max(jnp.where(live, degree, 0).astype(jnp.float32)).astype(jnp.int32)
    low = jnp.min(jnp.where(live, degree, last).astype(jnp.float32)).astype(jnp.int32)
    return low // LANES, top // LANES


def sums_kernel(orders, cols, trips, groups, wig_hbm, sky_hbm, col_hbm, ell_hbm, beam_hbm, out_ref, *scratch):
    wig_buf, tail_buf, sky_ref, col_ref, ell_ref, real_ref, imag_ref, table_ref = scratch[0:8]
    coeff_refs, sems, once = scratch[8:12], scratch[12], scratch[13]
    cycles = wig_hbm.shape[1]
    tiles = table_ref.shape[1] // LANES
    slot_tiles = col_ref.shape[0]
    rest = slot_tiles - trips * TRIP
    depth = wig_buf.shape[0]
    half = orders * cycles
    by_rows = 2 * half > MXU_ROWS

    def wig_copy(trip, slot):
        lanes = pl.ds(pl.multiple_of(trip * (TRIP * LANES), LANES), TRIP * LANES)
        return pltpu.make_async_copy(wig_hbm.at[:, :, lanes], wig_buf.at[slot], sems.at[slot])

    rest_lanes = pl.ds(trips * TRIP * LANES, rest * LANES)
    ell_copy = pltpu.make_async_copy(ell_hbm, ell_ref, once.at[0])
    col_copy = pltpu.make_async_copy(col_hbm, col_ref, once.at[1])
    real_copy = pltpu.make_async_copy(beam_hbm.at[:, 0, :], real_ref, once.at[2])
    imag_copy = pltpu.make_async_copy(beam_hbm.at[:, 1, :], imag_ref, once.at[3])
    sky_copy = pltpu.make_async_copy(sky_hbm, sky_ref, once.at[4])
    for copy in (real_copy, imag_copy, col_copy, ell_copy, sky_copy):
        copy.start()
    for trip in range(min(depth - 2, trips)):
        wig_copy(trip, trip).start()
    if rest:
        tail_copy = pltpu.make_async_copy(wig_hbm.at[:, :, rest_lanes], tail_buf, once.at[5])
        tail_copy.start()

    real_copy.wait()
    imag_copy.wait()
    most = pack_beam(real_ref, imag_ref, table_ref)
    unit = jnp.broadcast_to(most * (1.0 / FULL), (SUBLANES, LANES))
    col_copy.wait()
    ell_copy.wait()
    low, top = pick_span(col_ref, ell_ref, tiles)
    span = top - low + 1
    sky_copy.wait()
    row16 = lax.broadcasted_iota(jnp.int32, (16, LANES), 0).astype(jnp.float32).astype(jnp.bfloat16)

    def coeffs(count, first, tile, rows, coeff):
        degree = ell_ref[pl.ds(tile, rows), :]
        lanes = pl.ds(pl.multiple_of(tile * LANES, LANES), rows * LANES)
        sky_re = sky_ref[pl.ds(0, 1), lanes].reshape(rows, LANES) * unit[:rows]
        sky_im = sky_ref[pl.ds(1, 1), lanes].reshape(rows, LANES) * unit[:rows]
        high = (degree >> 7) - first
        index = degree & (LANES - 1)
        here = [high == t for t in range(1, count)]
        for order in range(orders):
            word = None
            for t in range(count):
                lanes = pl.ds(pl.multiple_of((first + t) * LANES, LANES), LANES)
                entry = jnp.broadcast_to(table_ref[pl.ds(order, 1), lanes], (rows, LANES))
                value = lane_pick(entry, index)
                word = value if t == 0 else jnp.where(here[t - 1], value, word)
            real = word.astype(jnp.float32)
            imag = (word << IMAG_SHIFT).astype(jnp.float32)
            power = jnp.exp2((word & (2**POWER_BITS - 1)).astype(jnp.float32) - float(LEAST_POWER + REAL_BITS))
            real, imag = real * power, imag * power
            coeff[order, pl.ds(0, rows), :] = sky_re * real - sky_im * imag
            coeff[orders + order, pl.ds(0, rows), :] = sky_re * imag + sky_im * real

    def values(wig, coeff, part, start, line):
        out = []
        for order in range(orders):
            here = wig[order, :, pl.ds(start, LANES)].astype(jnp.float32)
            row = coeff[part * orders + order, pl.ds(line, 1), :]
            out.append(here * jnp.broadcast_to(row, (cycles, LANES)))
        return jnp.concatenate(out, axis=0)

    def hot(tile):
        line = jnp.broadcast_to(col_ref[pl.ds(tile, 1), :], (16, LANES))
        away = line.astype(jnp.float32).astype(jnp.bfloat16) - row16
        one, zero = jnp.ones_like(away), jnp.zeros_like(away)
        out = [jnp.where(away == jnp.bfloat16(16 * g), one, zero) for g in range(cols // 16)]
        out += [zero] * (MXU // 16 - cols // 16)
        return jnp.concatenate(out, axis=0)

    def body(acc0, acc1):
        accs = (acc0, acc1)
        if by_rows:
            work = lambda i: [(0, i % 2, (0,)), (1, i % 2, (1,))]
        else:
            work = lambda i: [(i % 2, i // 2 % 2, (0, 1))]

        ahead = 2 if by_rows else 4

        def push(i, tile, count=2):
            left = hot(tile)
            right = hot(tile + 1) if count == 2 else jnp.zeros_like(left)
            both = jnp.concatenate([left, right], axis=1)
            for mxu, register, _ in work(i):
                pltpu.matmul_push_rhs(both, register, mxu, transpose=True)

        def multiply(i, wig, coeff, start, line, count=2):
            for mxu, register, parts in work(i):
                blocks = []
                for part in parts:
                    left = values(wig, coeff, part, start, line)
                    if count == 2:
                        right = values(wig, coeff, part, start + LANES, line + 1)
                    else:
                        right = jnp.zeros_like(left)
                    blocks.append(jnp.concatenate([left, right], axis=1))
                block = blocks[0] if len(blocks) == 1 else jnp.concatenate(blocks, axis=0)
                pltpu.matmul_acc_lhs(accs[mxu], block, load_staged_rhs=register)

        pairs = TRIP // 2
        tail_pairs = -(-rest // 2)

        def tail_size(i):
            return min(2, rest - 2 * i)

        def run(count, first):
            for which in range(TRIP // SUBLANES):
                coeffs(count, first, which * SUBLANES, SUBLANES, coeff_refs[which])
            for i in range(ahead):
                push(i, 2 * i)

            def trip_body(trip, turn, last):
                wig = wig_buf.at[lax.rem(trip, depth)]
                base = trip * TRIP
                now, later = coeff_refs[2 * turn : 2 * turn + 2], coeff_refs[2 - 2 * turn : 4 - 2 * turn]
                for i in range(pairs):
                    which = 2 * i // SUBLANES
                    if 2 * i % SUBLANES == 0:
                        lines = min(max(rest - which * SUBLANES, 0), SUBLANES) if last else SUBLANES
                        tile = base + TRIP + which * SUBLANES
                        if not last:
                            tile = pl.multiple_of(tile, SUBLANES)
                        if lines:
                            coeffs(count, first, tile, lines, later[which])
                    multiply(i, wig, now[which], 2 * i * LANES, 2 * i % SUBLANES)
                    after = i + ahead
                    if not last or after < pairs:
                        push(after, base + 2 * after)
                    elif after - pairs < tail_pairs:
                        push(after, base + 2 * after, tail_size(after - pairs))

            def arrived(trip):
                wig_copy(trip, lax.rem(trip, depth)).wait()

            def ask(trip):
                @pl.when(trip < trips)
                def _():
                    wig_copy(trip, lax.rem(trip, depth)).start()

            turns = (trips - 1) // 2
            if turns:

                @pl.loop(0, turns)
                def _(turn):
                    ask(2 * turn + depth - 2)
                    ask(2 * turn + depth - 1)
                    arrived(2 * turn)
                    arrived(2 * turn + 1)
                    trip_body(2 * turn, 0, False)
                    trip_body(2 * turn + 1, 1, False)

            for trip in range(2 * turns, trips):
                arrived(trip)
            if rest:
                tail_copy.wait()
            for trip in range(2 * turns, trips):
                trip_body(trip, trip % 2, trip == trips - 1)
            later = coeff_refs[2:4] if trips % 2 else coeff_refs[0:2]
            for i in range(tail_pairs):
                multiply(pairs + i, tail_buf, later[2 * i // SUBLANES], 2 * i * LANES, 2 * i % SUBLANES, tail_size(i))
                if ahead + i < tail_pairs:
                    tile = trips * TRIP + 2 * (i + ahead)
                    push(pairs + i + ahead, tile, tail_size(i + ahead))

        counts = sorted({min(c, tiles) for c in (4, 9)})
        below = 0
        for count in counts:
            first = jnp.minimum(low, tiles - count)

            @pl.when((span > below) & (span <= count) if below else span <= count)
            def _():
                run(count, first)

            below = count
        if below < tiles:

            @pl.when(span > below)
            def _():
                run(tiles, 0)

        width = out_ref.shape[2]
        sums = [pltpu.matmul_pop(acc0), pltpu.matmul_pop(acc1)]
        if not by_rows:
            sums = [sums[0] + sums[1]]
        sums = jnp.concatenate(sums, axis=0)
        for piece in range(cols // width):
            lanes = slice(piece * width, (piece + 1) * width)
            for cycle in range(cycles):
                if groups > 2 * orders:
                    pad = pl.ds(cycle * groups + 2 * orders, groups - 2 * orders)
                    out_ref[piece, pad, :] = jnp.zeros((groups - 2 * orders, width), jnp.float32)
            for row in range(2 * orders):
                for cycle in range(0, cycles, SUBLANES):
                    here = pl.ds(cycle * groups + row, SUBLANES, stride=groups)
                    start = row * cycles + cycle
                    out_ref[piece, here, :] = sums[start : start + SUBLANES, lanes]

    rows = half if by_rows else 2 * half
    pl.run_scoped(body, pltpu.ACC(0)((rows, MXU), jnp.float32), pltpu.ACC(1)((rows, MXU), jnp.float32))


def order_sums(wigner, sky_alm, beam_blm, slot_col, slot_ell, cols, groups):
    cycles, orders, slots = wigner.shape
    degrees = beam_blm.shape[2]
    tiles = slots // LANES
    trips = tiles // TRIP
    rest = tiles - trips * TRIP
    depth = 8
    width = min(cols, LANES)
    shape = (cols // width, cycles * groups, width)
    in_hbm = lambda x: pltpu.with_memory_space_constraint(x, pltpu.HBM)
    return pl.pallas_call(
        functools.partial(sums_kernel, orders, cols, trips, groups),
        out_shape=jax.ShapeDtypeStruct(shape, jnp.float32),
        in_specs=[pl.BlockSpec(memory_space=pltpu.HBM)] * 5,
        out_specs=pl.BlockSpec(memory_space=pltpu.VMEM),
        scratch_shapes=[
            pltpu.VMEM((depth, orders, cycles, TRIP * LANES), jnp.bfloat16),
            pltpu.VMEM((orders, cycles, max(rest, 1) * LANES), jnp.bfloat16),
            pltpu.VMEM((2, slots), jnp.float32),
            pltpu.VMEM((tiles, LANES), jnp.int32),
            pltpu.VMEM((tiles, LANES), jnp.int32),
            pltpu.VMEM((orders, degrees), jnp.float32),
            pltpu.VMEM((orders, degrees), jnp.float32),
            pltpu.VMEM((orders, degrees), jnp.int32),
            *[pltpu.VMEM((2 * orders, SUBLANES, LANES), jnp.float32) for _ in range(4)],
            pltpu.SemaphoreType.DMA((depth,)),
            pltpu.SemaphoreType.DMA((6,)),
        ],
        compiler_params=pltpu.CompilerParams(vmem_limit_bytes=32 * 1024 * 1024),
        name="order_sums",
    )(
        in_hbm(wigner.transpose(1, 0, 2)),
        in_hbm(sky_alm),
        in_hbm(slot_col.reshape(tiles, LANES)),
        in_hbm(slot_ell.reshape(tiles, LANES)),
        in_hbm(beam_blm.transpose(1, 0, 2)),
    )


def split(value):
    high = value.astype(jnp.bfloat16)
    return high, (value - high.astype(jnp.float32)).astype(jnp.bfloat16)


def split_table(table):
    high, low = split(jnp.asarray(table, jnp.float32))
    return jnp.stack([high, low])


def product(left, right):
    dot = functools.partial(jnp.dot, preferred_element_type=jnp.float32)
    return dot(left[0], right[0]) + dot(left[0], right[1]) + dot(left[1], right[0])


def line_step(orders, turns):
    step = 2 * orders
    while turns * step % SUBLANES:
        step += 1
    return step


def psi_rows(orders, blks, turns, samples):
    groups, lines = line_step(orders, turns), round_up(turns * samples, SUBLANES)
    table = np.zeros((blks, 2, lines, turns, groups))
    sample = np.arange(blks * samples).reshape(blks, samples)
    angle = 2.0 * np.pi * (sample[..., None] * np.arange(orders) % (blks * samples)) / (blks * samples)
    for turn in range(turns):
        rows = slice(turn * samples, (turn + 1) * samples)
        table[:, 0, rows, turn, :orders] = np.cos(angle)
        table[:, 0, rows, turn, orders : 2 * orders] = -np.sin(angle)
        table[:, 1, rows, turn, :orders] = np.sin(angle)
        table[:, 1, rows, turn, orders : 2 * orders] = np.cos(angle)
    return table.reshape(blks * 2 * lines, turns * groups)


def partner(me, step, size):
    if size & (size - 1):
        return lax.rem(me + step, size)
    for bit in range(size.bit_length() - 1):
        weight = 1 << bit
        if step & weight:
            me = me + weight * (1 - 2 * lax.rem(me // weight, 2))
    return me


def exchange_kernel(turns, lines, sums_ref, table_ref, order_ref, all_ref, from_ref, *scratch):
    recv, out, sum_send, sum_recv, all_send, all_recv = scratch
    ells, blks = lax.axis_size("ell"), lax.axis_size("blk")
    ell, blk = lax.axis_index("ell"), lax.axis_index("blk")
    pieces, _, width = sums_ref.shape
    rows = recv.shape[2]
    block = 2 * lines

    barrier = pltpu.get_barrier_semaphore()
    for step in range(1, ells):
        pl.semaphore_signal(barrier, inc=1, device_id={"ell": partner(ell, step, ells)}, device_id_type=MESH)
    for step in range(1, blks):
        pl.semaphore_signal(barrier, inc=1, device_id={"blk": partner(blk, step, blks)}, device_id_type=MESH)
    pl.semaphore_wait(barrier, ells + blks - 2)

    def sum_copy(piece, step):
        target = partner(ell, step, ells)
        return pltpu.make_async_remote_copy(
            src_ref=sums_ref.at[piece, pl.ds(pl.multiple_of(target * rows, SUBLANES), rows), :],
            dst_ref=recv.at[step - 1, piece],
            send_sem=sum_send.at[piece, step - 1],
            recv_sem=sum_recv.at[piece, step - 1],
            device_id={"ell": target},
            device_id_type=MESH,
        )

    def all_copy(piece, step):
        target = partner(blk, step, blks)
        return pltpu.make_async_remote_copy(
            src_ref=out.at[piece, pl.ds(pl.multiple_of(target * block, SUBLANES), block), :],
            dst_ref=all_ref.at[blk, piece],
            send_sem=all_send.at[piece, step - 1],
            recv_sem=all_recv.at[piece, step - 1],
            device_id={"blk": target},
            device_id_type=MESH,
        )

    for piece in range(pieces):
        for step in reversed(range(1, ells)):
            sum_copy(piece, step).start()

    order = order_ref[...]
    total = order.shape[1]
    first = from_ref.shape[0] * 2
    span = total // first
    place = (order % first) // 2
    lane = (order % 2) * span + order // first
    column = lax.broadcasted_iota(jnp.int32, (from_ref.shape[0], total), 1)
    here = lax.broadcasted_iota(jnp.int32, (from_ref.shape[0], total), 0) == place
    pick = lambda x: jnp.where(here, x, 0).astype(jnp.float32).astype(jnp.bfloat16)
    left = jnp.concatenate([pick(column // 16), pick(column % 16)], axis=0)
    right = lax.broadcasted_iota(jnp.int32, (LANES, total), 0) == lane
    right = right.astype(jnp.float32).astype(jnp.bfloat16)
    found = lax.dot_general(left, right, (((1,), (1,)), ((), ())), preferred_element_type=jnp.float32)
    half = from_ref.shape[0]
    from_ref[...] = (found[:half] * 16.0 + found[half:]).astype(jnp.int32)

    table = (table_ref[0], table_ref[1])
    for piece in range(pieces):
        total = sums_ref[piece, pl.ds(pl.multiple_of(ell * rows, SUBLANES), rows), :]
        for step in range(1, ells):
            sum_copy(piece, step).wait_recv()
            total = total + recv[step - 1, piece]
        out[piece] = product(table, split(total))
        for step in reversed(range(1, blks)):
            all_copy(piece, step).start()
        all_ref[blk, piece] = out[piece, pl.ds(pl.multiple_of(blk * block, SUBLANES), block), :]

    for piece in range(pieces):
        for step in range(1, blks):
            all_copy(piece, step).wait_recv()
    for piece in range(pieces):
        for step in range(1, ells):
            sum_copy(piece, step).wait_send()
        for step in range(1, blks):
            all_copy(piece, step).wait_send()


def exchange(sums, order_of_column, orders, cycles):
    ells, blks = lax.axis_size("ell"), lax.axis_size("blk")
    pieces, _, width = sums.shape
    turns, samples = cycles // ells, NPSI // blks
    lines = round_up(turns * samples, SUBLANES)
    rows = turns * line_step(orders, turns)
    total = order_of_column.shape[0]
    table = split_table(psi_rows(orders, blks, turns, samples))
    in_vmem = pl.BlockSpec(memory_space=pltpu.VMEM)
    return pl.pallas_call(
        functools.partial(exchange_kernel, turns, lines),
        out_shape=(
            jax.ShapeDtypeStruct((blks, pieces, 2 * lines, width), jnp.float32),
            jax.ShapeDtypeStruct((total // LANES, LANES), jnp.int32),
        ),
        in_specs=[in_vmem] * 3,
        out_specs=(in_vmem, in_vmem),
        scratch_shapes=[
            pltpu.VMEM((ells - 1, pieces, rows, width), jnp.float32),
            pltpu.VMEM((pieces, blks * 2 * lines, width), jnp.float32),
            pltpu.SemaphoreType.DMA((pieces, ells - 1)),
            pltpu.SemaphoreType.DMA((pieces, ells - 1)),
            pltpu.SemaphoreType.DMA((pieces, blks - 1)),
            pltpu.SemaphoreType.DMA((pieces, blks - 1)),
        ],
        compiler_params=pltpu.CompilerParams(
            collective_id=0, has_side_effects=True, vmem_limit_bytes=32 * 1024 * 1024
        ),
        name="exchange",
    )(sums, table, order_of_column[None, :])


def turned(value, turn, period):
    real, imag = value
    turn = turn % period
    if turn == 0:
        return real, imag
    if 4 * turn == period:
        return -imag, real
    cos, sin = math.cos(2.0 * math.pi * turn / period), math.sin(2.0 * math.pi * turn / period)
    return real * cos - imag * sin, real * sin + imag * cos


def transform(values):
    size = len(values)
    if size == 1:
        return values
    even, odd = transform(values[0::2]), transform(values[1::2])
    odd = [turned(value, j, size) for j, value in enumerate(odd)]
    low = [(e[0] + o[0], e[1] + o[1]) for e, o in zip(even, odd)]
    high = [(e[0] - o[0], e[1] - o[1]) for e, o in zip(even, odd)]
    return low + high


def phi_kernel(lines, all_ref, from_ref, table_ref, twist_ref, out_ref):
    turns, samples, _ = out_ref.shape
    blks, pieces, _, width = all_ref.shape
    places = from_ref.shape[0]
    per = LANES // width
    real, imag = [], []
    blocks = [(b, piece) for b in range(blks) for piece in range(pieces)]
    for tile in range(len(blocks) // per):
        for rows, into in ((pl.ds(0, lines), real), (pl.ds(lines, lines), imag)):
            part = [all_ref[b, piece, rows, :] for b, piece in blocks[tile * per : (tile + 1) * per]]
            into.append(part[0] if per == 1 else jnp.concatenate(part, axis=1))
    rows = []
    for place in range(places):
        source = jnp.broadcast_to(from_ref[pl.ds(place, 1), :], (lines, LANES))
        high, index = source >> 7, source & (LANES - 1)
        both = []
        for tiles in (real, imag):
            picked = lane_pick(tiles[0], index)
            for t in range(1, len(tiles)):
                picked = jnp.where(high == t, lane_pick(tiles[t], index), picked)
            both.append(picked)
        rows.append(jnp.concatenate(both, axis=1))
    first = product(split(jnp.concatenate(rows, axis=0)), (table_ref[0], table_ref[1]))
    values = []
    for place in range(places):
        here = first[place * lines : (place + 1) * lines]
        for side in range(2):
            re = here[:, 2 * side * LANES : (2 * side + 1) * LANES]
            im = here[:, (2 * side + 1) * LANES : (2 * side + 2) * LANES]
            cos = jnp.broadcast_to(twist_ref[0, pl.ds(2 * place + side, 1), :], (lines, LANES))
            sin = jnp.broadcast_to(twist_ref[1, pl.ds(2 * place + side, 1), :], (lines, LANES))
            values.append((re * cos - im * sin, re * sin + im * cos))
    for j, (value, _) in enumerate(transform(values)):
        for turn in range(turns):
            out_ref[turn, :, j * LANES : (j + 1) * LANES] = value[turn * samples : (turn + 1) * samples]


def phi_tables(degrees):
    outer = 2 * degrees // LANES
    span = degrees // outer
    angle = 2.0 * np.pi * np.outer(np.arange(span), np.arange(LANES)) / LANES
    table = np.zeros((2, 2, span, 2, 2, LANES))
    for side in range(2):
        table[0, side, :, side, 0] = np.cos(angle)
        table[0, side, :, side, 1] = np.sin(angle)
        table[1, side, :, side, 0] = -np.sin(angle)
        table[1, side, :, side, 1] = np.cos(angle)
    angle = 2.0 * np.pi * np.outer(np.arange(outer), np.arange(LANES)) / (2 * degrees)
    return table.reshape(4 * span, 4 * LANES), np.stack([np.cos(angle), np.sin(angle)])


def to_phi(gathered, origin, turns, samples, degrees):
    table, twist = phi_tables(degrees)
    in_vmem = pl.BlockSpec(memory_space=pltpu.VMEM)
    return pl.pallas_call(
        functools.partial(phi_kernel, gathered.shape[2] // 2),
        out_shape=jax.ShapeDtypeStruct((turns, samples, 2 * degrees), jnp.float32),
        in_specs=[in_vmem] * 4,
        out_specs=in_vmem,
        compiler_params=pltpu.CompilerParams(vmem_limit_bytes=32 * 1024 * 1024),
        name="to_phi",
    )(gathered, origin, split_table(table), jnp.asarray(twist, jnp.float32))


def on_device(wigner, sky_alm, beam_blm, slot_col, slot_ell, order_of_column):
    cycles, orders, _ = wigner.shape
    degrees = order_of_column.shape[0]
    ells, blks = lax.axis_size("ell"), lax.axis_size("blk")
    sums = order_sums(wigner, sky_alm, beam_blm, slot_col, slot_ell, degrees // blks, line_step(orders, cycles // ells))
    gathered, origin = exchange(sums, order_of_column, orders, cycles)
    return to_phi(gathered, origin, cycles // ells, NPSI // blks, degrees)


def solution(mesh):
    return jax.shard_map(
        on_device,
        mesh=mesh,
        in_specs=(
            P(None, None, ("ell", "blk")),
            P(None, ("ell", "blk")),
            P(),
            P(("ell", "blk")),
            P(("ell", "blk")),
            P(),
        ),
        out_specs=P("ell", "blk", None),
        check_vma=False,
    )
```
